256 devices in a mesh: row: 16 (over z_lo, y, core), col: 16 (over z_hi, x).
Axes of the slice: x: 4, y: 4, z: 8 (z_hi: 4, z_lo: 2; z = z_hi * 2 + z_lo), core: 2. Of those that a mesh axis runs over, the one named last changes fastest.
Arguments:
- tokens: bfloat16 [256, 2, 4096], P(None, None, 'row'), may hold values from -6 to 6
- task_emb: bfloat16 [512, 1024], replicated, may hold values from -6 to 6
- gen_in: bfloat16 [1024, 512], replicated, may hold values from -0.1875 to 0.1875
- gen_a: bfloat16 [512, 4096, 16], P(None, ('row', 'col')), may hold values from -0.0078125 to 0.0078125
- gen_b: bfloat16 [512, 16, 14336], P(None, 'row', 'col'), may hold values from -0.125 to 0.125
- w_gate: bfloat16 [4096, 14336], P('row', 'col'), may hold values from -0.09375 to 0.09375
- w_up: bfloat16 [4096, 14336], P('row', 'col'), may hold values from -0.09375 to 0.09375
- w_down: bfloat16 [14336, 4096], P('col', 'row'), may hold values from -0.046875 to 0.046875
- group_count: int32 [64], replicated, may hold values from 1 to 16, 256 in all
- group_task: int32 [64], replicated, may hold values from 0 to 511, as said below
Outputs:
- mixed: bfloat16 [256, 2, 4096], P('col', None, 'row')
The draws below stay inside these ranges and needn't reach their ends.
Inputs may be any that keep to these rules, and one draw needn't show every extreme that they name: `group_count`: requests in each group, in the order of the requests; they sum to 256 and the largest is 16. `group_task`: distinct task ids, one for each group.
All inputs are finite; a program needn't handle non-finite values.
Results may differ from the reference program's by a relative error of at most 0.0078.
Values may be sent and summed in bfloat16 or wider, within the bound.
A program may use at most 64 MiB of HBM per device.

```python
import math
import jax
import jax.numpy as jnp
import numpy as np

D = 4096
HIDDEN_UNITS = 14336
RANK = 16
EMB = 1024
HYPER = 512
TASKS = 512
GROUPS = 64
MOST = 16
REQUEST_COUNT = 256
DRAFT_TOKENS = 2


def draw_group_task(key, part):
    return jax.random.permutation(key, TASKS)[:GROUPS].astype(jnp.int32)


def block_levels(stream_key, shape, cuts, least, high):
    def one(dim, blocks):
        draws = jax.random.uniform(jax.random.fold_in(jax.random.fold_in(stream_key, 6), dim), (blocks,), jnp.float32, least / len(cuts), high / len(cuts))
        return jnp.repeat(jnp.exp(draws), shape[dim] // blocks).reshape((-1,) + (1,) * (len(shape) - dim - 1))

    level = one(*cuts[0])
    for cut in cuts[1:]:
        level = level * one(*cut)
    return level


def length_profile(number_of, total, limit, skew):
    weights = [(1 << 20) // math.isqrt(rank ** skew) + 1 for rank in range(2, number_of + 1)]
    rest, given = total - limit - (number_of - 1), [1] * (number_of - 1)
    while rest > 0:
        movable = [i for i in range(number_of - 1) if given[i] < limit]
        whole, budget = sum([weights[i] for i in movable]), rest
        for i in movable:
            addition = min(limit - given[i], max(1, budget * weights[i] // whole), rest)
            given[i] = given[i] + addition
            rest = rest - addition
    return np.array([limit] + given)


def uneven(own_key, number_of, total, limit, skew):
    if number_of == 2:
        one = jax.random.randint(own_key, (), max(1, total - limit), min(limit, total - 1) + 1)
        return jnp.stack([one, total - one])
    tallies = jnp.asarray(length_profile(number_of, total, limit, skew), jnp.int32)
    couples = (number_of - 1) // 2
    giver, sink = tallies[1:1 + 2 * couples:2], tallies[2:2 + 2 * couples:2]
    room = jnp.minimum(giver - 1, limit - sink)
    passed = jax.random.randint(jax.random.fold_in(own_key, 1), (couples,), 0, 1 << 20) % (room + 1)
    tallies = tallies.at[1:1 + 2 * couples:2].set(giver - passed).at[2:2 + 2 * couples:2].set(sink + passed)
    return tallies[jax.random.permutation(jax.random.fold_in(own_key, 2), number_of)]


def scatter_about(key, extent, width, reach, shards=(), kind=jnp.bfloat16):
    entries = jax.random.normal(key, extent, jnp.float32) * width
    if len(shards) > 0:
        entries = block_levels(key, extent, shards, -0.22, 0.18) * entries
    return jnp.clip(entries, min=-reach, max=reach).astype(kind)


def setup_inputs(seed: int = 0) -> dict:
    arg_keys = jax.random.split(jax.random.key(seed), 11)
    tokens = scatter_about(arg_keys[0], (REQUEST_COUNT, DRAFT_TOKENS, D), 1.0, 6.0, ((2, 16),))
    task_emb = scatter_about(arg_keys[1], (TASKS, EMB), 1.0, 6.0)
    gen_in = scatter_about(arg_keys[2], (EMB, HYPER), EMB ** -0.5, 0.1875)
    gen_a = scatter_about(arg_keys[3], (HYPER, D, RANK), (HYPER * D // 4) ** -0.5, 0.0078125, ((1, 256),))
    gen_b = scatter_about(arg_keys[4], (HYPER, RANK, HIDDEN_UNITS), (HYPER * RANK // 4) ** -0.5, 0.125, ((1, 16), (2, 16)))
    w_gate = scatter_about(arg_keys[5], (D, HIDDEN_UNITS), D ** -0.5, 0.09375, ((0, 16), (1, 16)))
    w_up = scatter_about(arg_keys[6], (D, HIDDEN_UNITS), D ** -0.5, 0.09375, ((0, 16), (1, 16)))
    w_down = scatter_about(arg_keys[7], (HIDDEN_UNITS, D), HIDDEN_UNITS ** -0.5, 0.046875, ((0, 16), (1, 16)))
    group_count = uneven(arg_keys[8], GROUPS, REQUEST_COUNT, MOST, 2).astype(jnp.int32)
    group_task = draw_group_task(jax.random.fold_in(arg_keys[10], 71), 0)
    return {"tokens": tokens, "task_emb": task_emb, "gen_in": gen_in, "gen_a": gen_a, "gen_b": gen_b, "w_gate": w_gate, "w_up": w_up, "w_down": w_down, "group_count": group_count, "group_task": group_task}


def reference(tokens, task_emb, gen_in, gen_a, gen_b, w_gate, w_up, w_down, group_count, group_task):
    group_ends = jnp.cumsum(group_count).astype(jnp.int32)
    request_ids = jnp.arange(REQUEST_COUNT, dtype=jnp.int32)
    request_group = jnp.sum((request_ids[:, None] >= group_ends[None, :]).astype(jnp.int32), axis=1).astype(jnp.int32)
    chosen = task_emb[group_task]
    hyper_out = jax.nn.silu(jnp.dot(chosen, gen_in, preferred_element_type=jnp.float32)).astype(jnp.bfloat16)
    factor_a = jnp.dot(hyper_out, gen_a.reshape(HYPER, D * RANK), preferred_element_type=jnp.float32).astype(jnp.bfloat16).reshape(GROUPS, D, RANK)
    second_factor = jnp.dot(hyper_out, gen_b.reshape(HYPER, RANK * HIDDEN_UNITS), preferred_element_type=jnp.float32).astype(jnp.bfloat16).reshape(GROUPS, RANK, HIDDEN_UNITS)
    flat_tokens = tokens.reshape(REQUEST_COUNT * DRAFT_TOKENS, D)
    gate_total = jnp.dot(flat_tokens, w_gate, preferred_element_type=jnp.float32)
    up_total = jnp.dot(flat_tokens, w_up, preferred_element_type=jnp.float32)
    reduced_rank_term = jnp.einsum("bsd,bdr->bsr", tokens.astype(jnp.float32), factor_a[request_group].astype(jnp.float32)).astype(jnp.bfloat16)
    adapter_update = jnp.einsum("klv,kve->kle", reduced_rank_term.astype(jnp.float32), second_factor[request_group].astype(jnp.float32))
    adapter_update = adapter_update.reshape(REQUEST_COUNT * DRAFT_TOKENS, HIDDEN_UNITS)
    hidden_state = (jax.nn.silu(gate_total) * (up_total + adapter_update)).astype(jnp.bfloat16)
    mixed = jnp.dot(hidden_state, w_down, preferred_element_type=jnp.float32).astype(jnp.bfloat16)
    return mixed.reshape(REQUEST_COUNT, DRAFT_TOKENS, D)
```

```python
import functools

import jax
import jax.numpy as jnp
from jax import lax
from jax.experimental import pallas as pl
from jax.experimental.pallas import tpu as pltpu
from jax.sharding import PartitionSpec as P

MESH = pl.DeviceIdType.MESH
F32 = jnp.float32
BF16 = jnp.bfloat16


def dot(a, b, dims=((1,), (0,))):
    return lax.dot_general(a, b, (dims, ((), ())), preferred_element_type=F32)


def kernel(
    tokens, task_emb, gen_in, gen_a, gen_b, w_gate, w_up, w_down, count, task,
    out,
    tok_v, emb_v, gin_v, ga_v, gb_v, wg_v, wu_v, wd_v, cnt_v, tsk_v,
    tokp_v, wgp_v, wup_v, wdp_v, b_v,
    low_s, low1_r, low1_s, low2_r,
    gate_s, up_s, gate_r, up_r, hid_v, mix_own, mix_par, mix_r,
    load_sem, pair_ss, pair_rs, l1_ss, l1_rs, l2_ss, l2_rs,
    g_ss, g_rs, u_ss, u_rs, h_ss, h_rs, m_ss, m_rs,
):
    row = lax.axis_index("row")
    col = lax.axis_index("col")
    chip = row // 2
    core = row % 2
    groups = count.shape[1]
    ranks = low_s.shape[1]

    bar = pltpu.get_barrier_semaphore()
    for j in range(1, 16):
        far = (col + j) % 16
        pl.semaphore_signal(bar, inc=1, device_id=((row + j) % 16, col), device_id_type=MESH)
        pl.semaphore_signal(bar, inc=1, device_id=(row, far), device_id_type=MESH)
        pl.semaphore_signal(bar, inc=1, device_id=(chip * 2 + 1 - core, far), device_id_type=MESH)

    loads = [
        pltpu.make_async_copy(src, dst, load_sem.at[n])
        for n, (src, dst) in enumerate(
            [
                (task, tsk_v), (task_emb, emb_v), (gen_in, gin_v), (count, cnt_v), (gen_a, ga_v),
                (tokens, tok_v), (gen_b, gb_v), (w_gate, wg_v), (w_up, wu_v), (w_down, wd_v),
            ]
        )
    ]
    for c in loads:
        c.start()

    def copy(src, dst, ss, rs, dev):
        return pltpu.make_async_remote_copy(
            src_ref=src, dst_ref=dst, send_sem=ss, recv_sem=rs, device_id=dev, device_id_type=MESH
        )

    gi = lax.broadcasted_iota(jnp.int32, (groups, groups), 0)
    gj = lax.broadcasted_iota(jnp.int32, (groups, groups), 1)
    loads[0].wait()
    task_of = jnp.sum(jnp.where(gi == gj, tsk_v[...].astype(F32), 0.0), axis=1, keepdims=True)
    tasks = emb_v.shape[0]
    pick = lax.broadcasted_iota(jnp.int32, (groups, tasks), 1).astype(F32) == task_of
    loads[1].wait()
    chosen = dot(jnp.where(pick, 1.0, 0.0).astype(BF16), emb_v[...]).astype(BF16)
    loads[2].wait()
    hyper = jax.nn.silu(dot(chosen, gin_v[...])).astype(BF16)

    loads[3].wait()
    cnt = cnt_v[...].astype(F32)
    ends = jnp.sum(jnp.where(gj <= gi, cnt, 0.0), axis=1, keepdims=True)
    starts = ends - jnp.sum(jnp.where(gj == gi, cnt, 0.0), axis=1, keepdims=True)

    def member(first, width):
        request = (lax.broadcasted_iota(jnp.int32, (groups, width), 1) + first) // 2
        request = request.astype(F32)
        return jnp.where((request >= starts) & (request < ends), 1.0, 0.0)

    loads[4].wait()
    fac_a = dot(ga_v[...], hyper, ((1,), (1,))).astype(BF16)
    n_tok = tok_v.shape[0]
    width = tok_v.shape[1]
    slab = fac_a.shape[0] // ranks
    a_of = dot(fac_a, member(0, n_tok).astype(BF16))
    which = lax.broadcasted_iota(jnp.int32, (slab * ranks, width), 0) // ranks + col * slab
    sel = jnp.where(lax.broadcasted_iota(jnp.int32, (slab * ranks, width), 1) == which, 1.0, 0.0)
    loads[5].wait()
    t_of = dot(sel.astype(BF16), tok_v[...], ((1,), (1,)))
    low = jnp.sum((a_of * t_of).reshape(slab, ranks, n_tok), axis=0)
    for h in range(2):
        for q in range(2):
            low_s[h, :, q, :] = low[:, h * 256 + q * 128 : h * 256 + q * 128 + 128]

    pl.semaphore_wait(bar, 45)

    l1 = []
    for j in range(1, 16):
        to = (row + j) % 16
        l1.append(
            copy(low_s.at[to % 2, pl.ds(to // 2 * 2, 2)], low1_r.at[j], l1_ss.at[j], l1_rs.at[j], (to, col))
        )
        l1[-1].start()
    mate = (chip * 2 + 1 - core, col)
    half = tok_v.shape[0] // 2
    other = pl.ds(pl.multiple_of((1 - core) * half, half), half)
    mine = pl.ds(pl.multiple_of(core * half, half), half)
    for n in (7, 8, 9):
        loads[n].wait()
    pair = [
        copy(tok_v.at[other], tokp_v, pair_ss.at[0], pair_rs.at[0], mate),
        copy(wg_v, wgp_v, pair_ss.at[1], pair_rs.at[1], mate),
        copy(wu_v, wup_v, pair_ss.at[2], pair_rs.at[2], mate),
        copy(wd_v, wdp_v, pair_ss.at[3], pair_rs.at[3], mate),
        copy(b_v.at[core], b_v.at[core], pair_ss.at[4], pair_rs.at[4], mate),
    ]
    for n in range(4):
        pair[n].start()
    loads[6].wait()
    b_v[core] = dot(hyper, gb_v[...]).astype(BF16)
    pair[4].start()

    gate = dot(tok_v[mine, :], wg_v[...])
    pair[0].wait_recv()
    pair[1].wait_recv()
    gate_s[...] = (gate + dot(tokp_v[...], wgp_v[...])).astype(BF16)
    share = half // 8

    def rows(i):
        return pl.ds(pl.multiple_of(i * share, share), share)

    def peer(j):
        return (chip + j) % 8

    gs = [
        copy(gate_s.at[rows(peer(j))], gate_r.at[j], g_ss.at[j], g_rs.at[j], (peer(j) * 2 + core, col))
        for j in range(1, 8)
    ]
    for c in gs:
        c.start()

    low1 = low_s[core, pl.ds(chip * 2, 2)]
    for j in range(1, 16):
        l1[j - 1].wait_recv()
        low1 = low1 + low1_r[j]
    low1_s[...] = low1
    l2 = []
    for j in range(1, 16):
        l2.append(copy(low1_s, low2_r.at[j], l2_ss.at[j], l2_rs.at[j], (row, (col + j) % 16)))
        l2[-1].start()

    up = dot(tok_v[mine, :], wu_v[...])
    pair[2].wait_recv()
    up = up + dot(tokp_v[...], wup_v[...])
    pair[4].wait_recv()
    for j in range(1, 16):
        l2[j - 1].wait_recv()
        low1 = low1 + low2_r[j]
    low1 = low1.astype(BF16).astype(F32)
    mem = member(core * half, half)
    spread = [
        (mem * jnp.concatenate([low1[a, 0:1, :], low1[a, 1:2, :]], axis=1)).astype(BF16) for a in range(2)
    ]
    b_all = b_v[...].reshape(2 * groups, b_v.shape[2])
    up = up + dot(jnp.concatenate(spread, axis=0), b_all, ((0,), (0,)))
    up_s[...] = up.astype(BF16)
    us = [
        copy(up_s.at[rows(peer(j))], up_r.at[j], u_ss.at[j], u_rs.at[j], (peer(j) * 2 + core, col))
        for j in range(1, 8)
    ]
    for c in us:
        c.start()

    gate_t = gate_s[rows(chip), :].astype(F32)
    for j in range(1, 8):
        gs[j - 1].wait_recv()
        gate_t = gate_t + gate_r[j].astype(F32)
    act = jax.nn.silu(gate_t)
    up_t = up_s[rows(chip), :].astype(F32)
    for j in range(1, 8):
        us[j - 1].wait_recv()
        up_t = up_t + up_r[j].astype(F32)
    hid_v[rows(chip), :] = (act * up_t).astype(BF16)

    hs = [
        copy(hid_v.at[rows(chip)], hid_v.at[rows(chip)], h_ss.at[j], h_rs.at[j], (peer(j) * 2 + core, col))
        for j in range(1, 8)
    ]
    for c in hs:
        c.start()
    pair[3].wait_recv()
    for j in range(1, 8):
        src = (chip + 8 - j) % 8
        copy(hid_v.at[rows(src)], hid_v.at[rows(src)], h_ss.at[j], h_rs.at[j], (row, col)).wait_recv()

    mix_own[...] = dot(hid_v[...], wd_v[...]).astype(BF16)
    mix_par[...] = dot(hid_v[...], wdp_v[...]).astype(BF16)
    own_half = col // 8 == core
    ms = []
    for j in range(8):
        b = (col + j) % 8
        to = core * 8 + b
        same = copy(mix_own.at[rows(b)], mix_r.at[col], m_ss.at[0, j], m_rs.at[col], (row, to))
        cross = copy(
            mix_par.at[rows(b)], mix_r.at[col], m_ss.at[1, j], m_rs.at[col], (chip * 2 + 1 - core, to)
        )
        ms.append((same, cross))
        if j == 0:
            pl.when(jnp.logical_not(own_half))(same.start)
        else:
            same.start()
        cross.start()

    @pl.when(own_half)
    def _():
        mix_r[col] = mix_own[rows(col % 8), :]

    for s in range(16):
        arrived = copy(mix_r.at[s], mix_r.at[s], m_ss.at[0, 0], m_rs.at[s], (row, col))
        pl.when(jnp.logical_not(own_half & (col == s)))(arrived.wait_recv)
    total = mix_r[0].astype(F32)
    for s in range(1, 16):
        total = total + mix_r[s].astype(F32)
    out[...] = total.astype(BF16)

    for c in l1 + l2 + pair + gs + us + hs:
        c.wait_send()
    for j in range(8):
        if j == 0:
            pl.when(jnp.logical_not(own_half))(ms[j][0].wait_send)
        else:
            ms[j][0].wait_send()
        ms[j][1].wait_send()


def shards(tokens, task_emb, gen_in, gen_a, gen_b, w_gate, w_up, w_down, group_count, group_task):
    batch, draft, width = tokens.shape
    hyper, slab, ranks = gen_a.shape
    groups = group_count.shape[0]
    units = w_gate.shape[1]
    n_tok = batch * draft
    half = n_tok // 2
    share = half // 8
    vm = pltpu.VMEM
    dma = pltpu.SemaphoreType.DMA
    args = (
        tokens.reshape(n_tok, width),
        task_emb,
        gen_in,
        gen_a.transpose(1, 2, 0).reshape(slab * ranks, hyper),
        gen_b.reshape(hyper, units),
        w_gate,
        w_up,
        w_down,
        group_count.reshape(1, groups),
        group_task.reshape(1, groups),
    )
    scratch = [vm(a.shape, a.dtype) for a in args]
    scratch += [
        vm((half, width), BF16),
        vm((width, units), BF16),
        vm((width, units), BF16),
        vm((units, width), BF16),
        vm((2, groups, units), BF16),
        vm((2, ranks, 2, half // 2), F32),
        vm((16, 2, 2, half // 2), F32),
        vm((2, 2, half // 2), F32),
        vm((16, 2, 2, half // 2), F32),
        vm((half, units), BF16),
        vm((half, units), BF16),
        vm((8, share, units), BF16),
        vm((8, share, units), BF16),
        vm((half, units), BF16),
        vm((half, width), BF16),
        vm((half, width), BF16),
        vm((16, share, width), BF16),
        dma((10,)), dma((5,)), dma((5,)), dma((16,)), dma((16,)), dma((16,)), dma((16,)),
        dma((8,)), dma((8,)), dma((8,)), dma((8,)), dma((8,)), dma((8,)), dma((2, 8)), dma((16,)),
    ]
    any_spec = pl.BlockSpec(memory_space=pl.ANY)
    out = pl.pallas_call(
        kernel,
        out_shape=jax.ShapeDtypeStruct((share, width), BF16),
        in_specs=[any_spec] * len(args),
        out_specs=pl.BlockSpec(memory_space=pltpu.VMEM),
        scratch_shapes=scratch,
        compiler_params=pltpu.CompilerParams(
            collective_id=0, has_side_effects=True, vmem_limit_bytes=56 * 1024 * 1024
        ),
    )(*args)
    return out.reshape(share // draft, draft, width)


def solution(mesh):
    placed = (
        P(None, None, "row"),
        P(),
        P(),
        P(None, ("row", "col"), None),
        P(None, "row", "col"),
        P("row", "col"),
        P("row", "col"),
        P("col", "row"),
        P(),
        P(),
    )
    return jax.shard_map(
        shards, mesh=mesh, in_specs=placed, out_specs=P("col", None, "row"), check_vma=False
    )
```

```python
import functools

import jax
import jax.numpy as jnp
from jax import lax
from jax.experimental import pallas as pl
from jax.experimental.pallas import tpu as pltpu
from jax.sharding import PartitionSpec as P

MESH = pl.DeviceIdType.MESH
F32 = jnp.float32
BF16 = jnp.bfloat16


def dot(a, b, dims=((1,), (0,))):
    return lax.dot_general(a, b, (dims, ((), ())), preferred_element_type=F32)


def kernel(
    tokens, task_emb, gen_in, gen_a, gen_b, w_gate, w_up, w_down, count, task,
    out,
    tok3_v, emb_v, gin_v, ga_v, gb_v, wg_v, wu_v, wd_v, cnt_v, tsk_v,
    tok_v, tokp_v, wgp_v, wup_v, wdp_v, b_v,
    low_s, low1_r, lowx_s, lowx_r, lowz_s, lowz_r,
    gate_s, up_s, gate_r, up_r, hid_v, mix_s, mix_r,
    load_sem, pair_ss, pair_rs, l1_ss, l1_rs, lx_ss, lx_rs, lz_ss, lz_rs,
    g_ss, g_rs, u_ss, u_rs, h_ss, h_rs, m_ss, m_rs,
):
    row = lax.axis_index("row")
    col = lax.axis_index("col")
    z_lo, y, core = row // 8, row // 2 % 4, row % 2
    z_hi, x = col // 4, col % 4
    chip = row // 2
    groups = count.shape[1]
    ranks = low_s.shape[1]
    mate = (row + 1 - 2 * core, col)

    def in_row(dz, dy, dk, sign=1):
        return ((z_lo + dz) % 2 * 4 + (y + sign * dy + 4) % 4) * 2 + (core + dk) % 2

    def in_col(dz, dx):
        return (z_hi + dz) % 4 * 4 + (x + dx) % 4

    row_steps = [(dz, dy, dk) for dz in (1, 0) for dy in (2, 1, 3, 0) for dk in (1, 0)][:-1]
    chip_steps = [(dz, dy) for dz in (1, 0) for dy in (2, 1, 3, 0)][:-1]

    bar = pltpu.get_barrier_semaphore()
    for d in (2, 1, 3):
        pl.semaphore_signal(bar, inc=1, device_id=(row, in_col(d, 0)), device_id_type=MESH)
    for step in row_steps:
        pl.semaphore_signal(bar, inc=1, device_id=(in_row(*step), col), device_id_type=MESH)
    for d in (2, 1, 3):
        pl.semaphore_signal(bar, inc=1, device_id=(row, in_col(0, d)), device_id_type=MESH)

    loads = [
        pltpu.make_async_copy(src, dst, load_sem.at[n])
        for n, (src, dst) in enumerate(
            [
                (task, tsk_v), (task_emb, emb_v), (gen_in, gin_v), (count, cnt_v), (gen_a, ga_v),
                (tokens, tok3_v), (gen_b, gb_v), (w_gate, wg_v), (w_up, wu_v), (w_down, wd_v),
            ]
        )
    ]
    for c in loads:
        c.start()

    def copy(src, dst, ss, rs, dev):
        return pltpu.make_async_remote_copy(
            src_ref=src, dst_ref=dst, send_sem=ss, recv_sem=rs, device_id=dev, device_id_type=MESH
        )

    gi = lax.broadcasted_iota(jnp.int32, (groups, groups), 0)
    gj = lax.broadcasted_iota(jnp.int32, (groups, groups), 1)
    loads[0].wait()
    task_of = jnp.sum(jnp.where(gi == gj, tsk_v[...].astype(F32), 0.0), axis=1, keepdims=True)
    tasks = emb_v.shape[0]
    pick = lax.broadcasted_iota(jnp.int32, (groups, tasks), 1).astype(F32) == task_of
    loads[1].wait()
    chosen = dot(jnp.where(pick, 1.0, 0.0).astype(BF16), emb_v[...]).astype(BF16)
    loads[2].wait()
    hyper = jax.nn.silu(dot(chosen, gin_v[...])).astype(BF16)

    loads[3].wait()
    cnt = cnt_v[...].astype(F32)
    ends = jnp.sum(jnp.where(gj <= gi, cnt, 0.0), axis=1, keepdims=True)
    starts = ends - jnp.sum(jnp.where(gj == gi, cnt, 0.0), axis=1, keepdims=True)

    def member(first, width):
        request = (lax.broadcasted_iota(jnp.int32, (groups, width), 1) + first) // 2
        request = request.astype(F32)
        return jnp.where((request >= starts) & (request < ends), 1.0, 0.0)

    loads[4].wait()
    fac_a = dot(ga_v[...], hyper, ((1,), (1,))).astype(BF16)
    n_tok = tok_v.shape[0]
    width = tok_v.shape[1]
    slab = fac_a.shape[0] // ranks
    a_of = dot(fac_a, member(0, n_tok).astype(BF16))
    which = lax.broadcasted_iota(jnp.int32, (slab * ranks, width), 0) // ranks + col * slab
    sel = jnp.where(lax.broadcasted_iota(jnp.int32, (slab * ranks, width), 1) == which, 1.0, 0.0)
    loads[5].wait()
    tok_v[...] = tok3_v[...].reshape(n_tok, width)
    t_of = dot(sel.astype(BF16), tok_v[...], ((1,), (1,)))
    low = jnp.sum((a_of * t_of).reshape(slab, ranks, n_tok), axis=0)
    for h in range(2):
        for q in range(2):
            low_s[h, :, q, :] = low[:, h * 256 + q * 128 : h * 256 + q * 128 + 128]

    pl.semaphore_wait(bar, 21)

    l1 = []
    for n, (dz, dy, dk) in enumerate(row_steps):
        to = in_row(dz, dy, dk)
        l1.append(
            copy(low_s.at[to % 2, pl.ds(to // 2 * 2, 2)], low1_r.at[n], l1_ss.at[n], l1_rs.at[n], (to, col))
        )
        l1[-1].start()
    half = tok_v.shape[0] // 2
    other = pl.ds(pl.multiple_of((1 - core) * half, half), half)
    mine = pl.ds(pl.multiple_of(core * half, half), half)
    for n in (7, 8, 9):
        loads[n].wait()
    pair = [
        copy(tok_v.at[other], tokp_v, pair_ss.at[0], pair_rs.at[0], mate),
        copy(wg_v, wgp_v, pair_ss.at[1], pair_rs.at[1], mate),
        copy(wu_v, wup_v, pair_ss.at[2], pair_rs.at[2], mate),
        copy(wd_v, wdp_v, pair_ss.at[3], pair_rs.at[3], mate),
        copy(b_v.at[core], b_v.at[core], pair_ss.at[4], pair_rs.at[4], mate),
    ]
    for n in range(4):
        pair[n].start()
    loads[6].wait()
    b_v[core] = dot(hyper, gb_v[...]).astype(BF16)
    pair[4].start()

    gate = dot(tok_v[mine, :], wg_v[...])
    pair[0].wait_recv()
    pair[1].wait_recv()
    gate_s[...] = (gate + dot(tokp_v[...], wgp_v[...])).astype(BF16)
    share = half // 8
    part = share // 2

    def rows(i, first=0, size=share):
        return pl.ds(pl.multiple_of(i * share + first, size), size)

    def peer(dz, dy, sign=1):
        return in_row(dz, dy, 0, sign) // 2

    gs = []
    for n, (dz, dy) in enumerate(chip_steps):
        i = peer(dz, dy)
        gs.append(copy(gate_s.at[rows(i)], gate_r.at[n], g_ss.at[n], g_rs.at[n], (i * 2 + core, col)))
    for n, (dz, dy) in enumerate(chip_steps):
        if dz == 0:
            gs[n].start()

    low1 = low_s[core, pl.ds(chip * 2, 2)]
    for n in range(15):
        l1[n].wait_recv()
        low1 = low1 + low1_r[n]
    lowx_s[...] = low1
    lx = [
        copy(lowx_s, lowx_r.at[n], lx_ss.at[n], lx_rs.at[n], (row, in_col(0, d)))
        for n, d in enumerate((2, 1, 3))
    ]
    for c in lx:
        c.start()
    up = dot(tok_v[mine, :], wu_v[...])
    for n in range(3):
        lx[n].wait_recv()
        low1 = low1 + lowx_r[n]
    lowz_s[...] = low1
    lz = [
        copy(lowz_s, lowz_r.at[n], lz_ss.at[n], lz_rs.at[n], (row, in_col(d, 0)))
        for n, d in enumerate((2, 1, 3))
    ]
    for c in lz:
        c.start()
    for n, (dz, dy) in enumerate(chip_steps):
        if dz == 1:
            gs[n].start()

    pair[2].wait_recv()
    up = up + dot(tokp_v[...], wup_v[...])
    pair[4].wait_recv()
    mem = member(core * half, half)
    b_all = b_v[...].reshape(2 * groups, b_v.shape[2])
    for n in range(3):
        lz[n].wait_recv()
        low1 = low1 + lowz_r[n]
    low1 = low1.astype(BF16).astype(F32)
    spread = [
        (mem * jnp.concatenate([low1[a, 0:1, :], low1[a, 1:2, :]], axis=1)).astype(BF16) for a in range(2)
    ]
    up = up + dot(jnp.concatenate(spread, axis=0), b_all, ((0,), (0,)))
    up_s[...] = up.astype(BF16)
    us = []
    for a in range(2):
        us.append([])
        for n, (dz, dy) in enumerate(chip_steps):
            i = peer(dz, dy)
            us[a].append(
                copy(
                    up_s.at[rows(i, a * part, part)], up_r.at[a, n], u_ss.at[a, n], u_rs.at[a, n],
                    (i * 2 + core, col),
                )
            )
            us[a][-1].start()

    gate_t = gate_s[rows(chip), :].astype(F32)
    for n in range(7):
        gs[n].wait_recv()
        gate_t = gate_t + gate_r[n].astype(F32)
    act = jax.nn.silu(gate_t)
    hs = []
    for a in range(2):
        up_t = up_s[rows(chip, a * part, part), :].astype(F32)
        for n in range(7):
            us[a][n].wait_recv()
            up_t = up_t + up_r[a, n].astype(F32)
        hid_v[a, chip] = (act[a * part : a * part + part] * up_t).astype(BF16)
        hs.append([])
        for n, (dz, dy) in enumerate(chip_steps):
            hs[a].append(
                copy(
                    hid_v.at[a, chip], hid_v.at[a, chip], h_ss.at[a, n], h_rs.at[a, n],
                    (peer(dz, dy) * 2 + core, col),
                )
            )
            hs[a][-1].start()

    pair[3].wait_recv()
    own_half = col // 8 == core
    d = (z_hi - 2 * core + 4) % 4
    far = 1 - (d + 1) // 2 % 2
    ms = []
    for a in range(2):
        for n, (dz, dy) in enumerate(chip_steps):
            src = peer(dz, dy, -1)
            copy(hid_v.at[a, src], hid_v.at[a, src], h_ss.at[a, n], h_rs.at[a, n], (row, col)).wait_recv()
        hid = hid_v[a].reshape(8 * part, hid_v.shape[3])
        mix_s[a, 0] = dot(hid, wd_v[...]).astype(BF16).reshape(8, part, width)
        mix_s[a, 1] = dot(hid, wdp_v[...]).astype(BF16).reshape(8, part, width)
        for t in range(2):
            for n, dx in enumerate((2, 1, 3, 0)):
                b = (far + t) % 2 * 4 + (x + dx) % 4
                to = core * 8 + b
                cross = copy(
                    mix_s.at[a, 1, b], mix_r.at[a, col], m_ss.at[a, t, n, 1], m_rs.at[a, col], (mate[0], to)
                )
                cross.start()
                same = copy(
                    mix_s.at[a, 0, b], mix_r.at[a, col], m_ss.at[a, t, n, 0], m_rs.at[a, col], (row, to)
                )
                local = t == 1 and dx == 0
                if local:
                    pl.when(jnp.logical_not(own_half))(same.start)
                else:
                    same.start()
                ms.append((cross, same, local))

        @pl.when(own_half)
        def _():
            mix_r[a, col] = mix_s[a, 0, col % 8]

    for a in range(2):
        for s in range(16):
            arrived = copy(mix_r.at[a, s], mix_r.at[a, s], m_ss.at[a, 0, 0, 0], m_rs.at[a, s], (row, col))
            pl.when(jnp.logical_not(own_half & (col == s)))(arrived.wait_recv)
        total = mix_r[a, 0].astype(F32)
        for s in range(1, 16):
            total = total + mix_r[a, s].astype(F32)
        out[pl.ds(a * part, part), :] = total.astype(BF16)

    for c in l1 + lx + lz + pair + gs + us[0] + us[1] + hs[0] + hs[1]:
        c.wait_send()
    for cross, same, local in ms:
        cross.wait_send()
        if local:
            pl.when(jnp.logical_not(own_half))(same.wait_send)
        else:
            same.wait_send()


def shards(tokens, task_emb, gen_in, gen_a, gen_b, w_gate, w_up, w_down, group_count, group_task):
    batch, draft, width = tokens.shape
    hyper, slab, ranks = gen_a.shape
    groups = group_count.shape[0]
    units = w_gate.shape[1]
    n_tok = batch * draft
    half = n_tok // 2
    share = half // 8
    part = share // 2
    vm = pltpu.VMEM
    dma = pltpu.SemaphoreType.DMA
    args = (
        tokens,
        task_emb,
        gen_in,
        gen_a.transpose(1, 2, 0).reshape(slab * ranks, hyper),
        gen_b.reshape(hyper, units),
        w_gate,
        w_up,
        w_down,
        group_count.reshape(1, groups),
        group_task.reshape(1, groups),
    )
    scratch = [vm(a.shape, a.dtype) for a in args]
    scratch += [
        vm((n_tok, width), BF16),
        vm((half, width), BF16),
        vm((width, units), BF16),
        vm((width, units), BF16),
        vm((units, width), BF16),
        vm((2, groups, units), BF16),
        vm((2, ranks, 2, half // 2), F32),
        vm((15, 2, 2, half // 2), F32),
        vm((2, 2, half // 2), F32),
        vm((3, 2, 2, half // 2), F32),
        vm((2, 2, half // 2), F32),
        vm((3, 2, 2, half // 2), F32),
        vm((half, units), BF16),
        vm((half, units), BF16),
        vm((7, share, units), BF16),
        vm((2, 7, part, units), BF16),
        vm((2, 8, part, units), BF16),
        vm((2, 2, 8, part, width), BF16),
        vm((2, 16, part, width), BF16),
    ]
    scratch += [
        dma(n)
        for n in (
            (10,), (5,), (5,), (15,), (15,), (3,), (3,), (3,), (3,),
            (7,), (7,), (2, 7), (2, 7), (2, 7), (2, 7), (2, 2, 4, 2), (2, 16),
        )
    ]
    any_spec = pl.BlockSpec(memory_space=pl.ANY)
    out = pl.pallas_call(
        kernel,
        out_shape=jax.ShapeDtypeStruct((share, width), BF16),
        in_specs=[any_spec] * len(args),
        out_specs=pl.BlockSpec(memory_space=pltpu.VMEM),
        scratch_shapes=scratch,
        compiler_params=pltpu.CompilerParams(
            collective_id=0, has_side_effects=True, vmem_limit_bytes=56 * 1024 * 1024
        ),
    )(*args)
    return out.reshape(share // draft, draft, width)


def solution(mesh):
    placed = (
        P(None, None, "row"),
        P(),
        P(),
        P(None, ("row", "col"), None),
        P(None, "row", "col"),
        P("row", "col"),
        P("row", "col"),
        P("col", "row"),
        P(),
        P(),
    )
    return jax.shard_map(
        shards, mesh=mesh, in_specs=placed, out_specs=P("col", None, "row"), check_vma=False
    )
```

```python
import functools

import jax
import jax.numpy as jnp
from jax import lax
from jax.experimental import pallas as pl
from jax.experimental.pallas import tpu as pltpu
from jax.sharding import PartitionSpec as P

MESH = pl.DeviceIdType.MESH
F32 = jnp.float32
BF16 = jnp.bfloat16


def dot(a, b, dims=((1,), (0,))):
    return lax.dot_general(a, b, (dims, ((), ())), preferred_element_type=F32)


def kernel(
    tokens, task_emb, gen_in, gen_a, gen_b, w_gate, w_up, w_down, count, task,
    out,
    tok3_v, emb_v, gin_v, ga_v, gb_v, wg_v, wu_v, wd_v, cnt_v, tsk_v,
    tok_v, tokp_v, wgp_v, wup_v, wdp_v, b_v,
    low_s, low1_r, low2_s, low2_r,
    gate_s, up_f, up_s, gate_r, up_r, hid_v, mix_f, mix_s, mix_r, end_s, end_r,
    known, load_sem, pair_ss, pair_rs, l1_ss, l1_rs, l2_ss, l2_rs,
    g_ss, g_rs, u_ss, u_rs, h_ss, h_rs, m_ss, m_rs, e_ss, e_rs,
):
    row = lax.axis_index("row")
    col = lax.axis_index("col")
    z_lo, y, core = row // 8, row // 2 % 4, row % 2
    z_hi, x = col // 4, col % 4
    chip = row // 2
    groups = count.shape[1]
    ranks = low_s.shape[1]
    mate = (row + 1 - 2 * core, col)

    def in_row(dz, dy, dk, sign=1):
        return ((z_lo + dz) % 2 * 4 + (y + sign * dy + 4) % 4) * 2 + (core + dk) % 2

    def in_col(dz, dx):
        return (z_hi + dz) % 4 * 4 + (x + dx) % 4

    row_steps = [(dz, dy, dk) for dz in (1, 0) for dy in (2, 1, 3, 0) for dk in (1, 0)][:-1]
    col_steps = [(dz, dx) for dz in (2, 1, 3, 0) for dx in (2, 1, 3, 0)][:-1]
    chip_steps = [(dz, dy) for dz in (1, 0) for dy in (2, 1, 3, 0)][:-1]

    bar = pltpu.get_barrier_semaphore()
    for d in (2, 1, 3):
        pl.semaphore_signal(bar, inc=1, device_id=(row, in_col(d, 0)), device_id_type=MESH)
    for step in row_steps:
        pl.semaphore_signal(bar, inc=1, device_id=(in_row(*step), col), device_id_type=MESH)
    for d in (2, 1, 3):
        pl.semaphore_signal(bar, inc=1, device_id=(row, in_col(0, d)), device_id_type=MESH)

    loads = [
        pltpu.make_async_copy(src, dst, load_sem.at[n])
        for n, (src, dst) in enumerate(
            [
                (task, tsk_v), (task_emb, emb_v), (gen_in, gin_v), (count, cnt_v), (gen_a, ga_v),
                (tokens, tok3_v), (gen_b, gb_v), (w_gate, wg_v), (w_up, wu_v), (w_down, wd_v),
            ]
        )
    ]
    for c in loads:
        c.start()

    def copy(src, dst, ss, rs, dev):
        return pltpu.make_async_remote_copy(
            src_ref=src, dst_ref=dst, send_sem=ss, recv_sem=rs, device_id=dev, device_id_type=MESH
        )

    gi = lax.broadcasted_iota(jnp.int32, (groups, groups), 0)
    gj = lax.broadcasted_iota(jnp.int32, (groups, groups), 1)
    loads[0].wait()
    task_of = jnp.sum(jnp.where(gi == gj, tsk_v[...].astype(F32), 0.0), axis=1, keepdims=True)
    tasks = emb_v.shape[0]
    pick = lax.broadcasted_iota(jnp.int32, (groups, tasks), 1).astype(F32) == task_of
    loads[1].wait()
    chosen = dot(jnp.where(pick, 1.0, 0.0).astype(BF16), emb_v[...]).astype(BF16)
    loads[2].wait()
    hyper = jax.nn.silu(dot(chosen, gin_v[...])).astype(BF16)

    loads[3].wait()
    cnt = cnt_v[...].astype(F32)
    ends = jnp.sum(jnp.where(gj <= gi, cnt, 0.0), axis=1, keepdims=True)
    starts = ends - jnp.sum(jnp.where(gj == gi, cnt, 0.0), axis=1, keepdims=True)

    def member(first, width):
        request = (lax.broadcasted_iota(jnp.int32, (groups, width), 1) + first) // 2
        request = request.astype(F32)
        return jnp.where((request >= starts) & (request < ends), 1.0, 0.0)

    loads[4].wait()
    fac_a = dot(ga_v[...], hyper, ((1,), (1,))).astype(BF16)
    n_tok = tok_v.shape[0]
    width = tok_v.shape[1]
    slab = fac_a.shape[0] // ranks
    a_of = dot(fac_a, member(0, n_tok).astype(BF16))
    which = lax.broadcasted_iota(jnp.int32, (slab * ranks, width), 0) // ranks + col * slab
    sel = jnp.where(lax.broadcasted_iota(jnp.int32, (slab * ranks, width), 1) == which, 1.0, 0.0)
    loads[5].wait()
    tok_v[...] = tok3_v[...].reshape(n_tok, width)
    t_of = dot(sel.astype(BF16), tok_v[...], ((1,), (1,)))
    low = jnp.sum((a_of * t_of).reshape(slab, ranks, n_tok), axis=0)
    for h in range(2):
        for q in range(2):
            low_s[h, :, q, :] = low[:, h * 256 + q * 128 : h * 256 + q * 128 + 128]

    pl.semaphore_wait(bar, 21)
    for d in (2, 1, 3):
        pl.semaphore_signal(known, inc=1, device_id=(row, in_col(d, 0)), device_id_type=MESH)

    l1 = []
    for n, (dz, dy, dk) in enumerate(row_steps):
        to = in_row(dz, dy, dk)
        l1.append(
            copy(low_s.at[to % 2, pl.ds(to // 2 * 2, 2)], low1_r.at[n], l1_ss.at[n], l1_rs.at[n], (to, col))
        )
        l1[-1].start()
    half = tok_v.shape[0] // 2
    other = pl.ds(pl.multiple_of((1 - core) * half, half), half)
    mine = pl.ds(pl.multiple_of(core * half, half), half)
    for n in (7, 8, 9):
        loads[n].wait()
    pair = [
        copy(tok_v.at[other], tokp_v, pair_ss.at[0], pair_rs.at[0], mate),
        copy(wg_v, wgp_v, pair_ss.at[1], pair_rs.at[1], mate),
        copy(wu_v, wup_v, pair_ss.at[2], pair_rs.at[2], mate),
        copy(wd_v, wdp_v, pair_ss.at[3], pair_rs.at[3], mate),
        copy(b_v.at[core], b_v.at[core], pair_ss.at[4], pair_rs.at[4], mate),
    ]
    for n in range(4):
        pair[n].start()
    loads[6].wait()
    b_v[core] = dot(hyper, gb_v[...]).astype(BF16)
    pair[4].start()

    gate = dot(tok_v[mine, :], wg_v[...])
    pair[0].wait_recv()
    pair[1].wait_recv()
    share = half // 8
    part = share // 2
    units = gate.shape[1]
    gate_s[...] = (gate + dot(tokp_v[...], wgp_v[...])).astype(BF16).reshape(2, 8, part, units)

    def peer(dz, dy, sign=1):
        return in_row(dz, dy, 0, sign) // 2

    gs = []
    for n, (dz, dy) in enumerate(chip_steps):
        i = peer(dz, dy)
        gs.append(copy(gate_s.at[:, i], gate_r.at[n], g_ss.at[n], g_rs.at[n], (i * 2 + core, col)))
    for n, (dz, dy) in enumerate(chip_steps):
        if dz == 0:
            gs[n].start()

    low = low_s[core, pl.ds(chip * 2, 2)]
    for n in range(15):
        l1[n].wait_recv()
        low = low + low1_r[n]
    low2_s[...] = low
    pl.semaphore_wait(known, 3)
    l2 = []
    for n, (dz, dx) in enumerate(col_steps):
        l2.append(copy(low2_s, low2_r.at[n], l2_ss.at[n], l2_rs.at[n], (row, in_col(dz, dx))))
        l2[-1].start()
    for n, (dz, dy) in enumerate(chip_steps):
        if dz == 1:
            gs[n].start()

    up = dot(tok_v[mine, :], wu_v[...])
    pair[2].wait_recv()
    up_f[...] = up + dot(tokp_v[...], wup_v[...])
    pair[4].wait_recv()
    b_all = b_v[...].reshape(2 * groups, units)
    block = half // 2
    mem = [member(core * half + a * block, block) for a in range(2)]
    for n in range(15):
        l2[n].wait_recv()
        low = low + low2_r[n]
    low = low.astype(BF16).astype(F32)
    us = []
    for a in range(2):
        spread = jnp.concatenate([mem[a] * low[r, a : a + 1, :] for r in range(2)], axis=0).astype(BF16)
        up = up_f[a * block : a * block + block, :] + dot(spread, b_all, ((0,), (0,)))
        up_s[a] = up.astype(BF16).reshape(8, part, units)
        us.append([])
        for n, (dz, dy) in enumerate(chip_steps):
            i = peer(dz, dy)
            us[a].append(
                copy(up_s.at[a, i], up_r.at[a, n], u_ss.at[a, n], u_rs.at[a, n], (i * 2 + core, col))
            )
            us[a][-1].start()

    for n in range(7):
        gs[n].wait_recv()
    hs = []
    for a in range(2):
        gate = gate_s[a, chip].astype(F32)
        for n in range(7):
            gate = gate + gate_r[n, a].astype(F32)
        act = jax.nn.silu(gate)
        up = up_s[a, chip].astype(F32)
        for n in range(7):
            us[a][n].wait_recv()
            up = up + up_r[a, n].astype(F32)
        hid_v[a, chip] = (act * up).astype(BF16)
        hs.append([])
        for n, (dz, dy) in enumerate(chip_steps):
            hs[a].append(
                copy(
                    hid_v.at[a, chip], hid_v.at[a, chip], h_ss.at[a, n], h_rs.at[a, n],
                    (peer(dz, dy) * 2 + core, col),
                )
            )
            hs[a][-1].start()

    pair[3].wait_recv()
    ms = []
    for a in range(2):
        for n, (dz, dy) in enumerate(chip_steps):
            src = peer(dz, dy, -1)
            copy(hid_v.at[a, src], hid_v.at[a, src], h_ss.at[a, n], h_rs.at[a, n], (row, col)).wait_recv()
        hid = hid_v[a].reshape(block, units)
        for k, w in enumerate((wd_v, wdp_v)):
            mix = dot(hid, w[...])
            mix_f[a, k] = mix.reshape(4, share, width)
            mix_s[a, k] = mix.astype(BF16).reshape(4, share, width)
        ms.append([])
        for n, d in enumerate((2, 1, 3)):
            ms[a].append(
                copy(mix_s.at[a, :, (x + d) % 4], mix_r.at[a, n], m_ss.at[a, n], m_rs.at[a, n], (row, in_col(0, d)))
            )
            ms[a][-1].start()
    es = []
    for a in range(2):
        to = 2 * core + a
        here = z_hi == to
        mix = mix_f[a, :, x]
        for n in range(3):
            ms[a][n].wait_recv()
            mix = mix + mix_r[a, n].astype(F32)
        end_s[a] = mix.astype(BF16)
        cross = copy(end_s.at[a, 1], end_r.at[z_hi], e_ss.at[a, 1], e_rs.at[z_hi], (mate[0], to * 4 + x))
        same = copy(end_s.at[a, 0], end_r.at[z_hi], e_ss.at[a, 0], e_rs.at[z_hi], (row, to * 4 + x))
        pl.when(jnp.logical_not(here))(same.start)
        cross.start()

        @pl.when(here)
        def _():
            end_r[z_hi] = end_s[a, 0]

        es.append((same, cross, here))

    mine = z_hi // 2 == core
    for s in range(4):
        arrived = copy(end_r.at[s], end_r.at[s], e_ss.at[0, 0], e_rs.at[s], (row, col))
        pl.when(jnp.logical_not(mine & (z_hi == s)))(arrived.wait_recv)
    total = end_r[0].astype(F32)
    for s in range(1, 4):
        total = total + end_r[s].astype(F32)
    out[...] = total.astype(BF16)

    for c in l1 + l2 + pair + gs + us[0] + us[1] + hs[0] + hs[1] + ms[0] + ms[1]:
        c.wait_send()
    for same, cross, here in es:
        pl.when(jnp.logical_not(here))(same.wait_send)
        cross.wait_send()


def shards(tokens, task_emb, gen_in, gen_a, gen_b, w_gate, w_up, w_down, group_count, group_task):
    batch, draft, width = tokens.shape
    hyper, slab, ranks = gen_a.shape
    groups = group_count.shape[0]
    units = w_gate.shape[1]
    n_tok = batch * draft
    half = n_tok // 2
    share = half // 8
    part = share // 2
    vm = pltpu.VMEM
    dma = pltpu.SemaphoreType.DMA
    args = (
        tokens,
        task_emb,
        gen_in,
        gen_a.transpose(1, 2, 0).reshape(slab * ranks, hyper),
        gen_b.reshape(hyper, units),
        w_gate,
        w_up,
        w_down,
        group_count.reshape(1, groups),
        group_task.reshape(1, groups),
    )
    scratch = [vm(a.shape, a.dtype) for a in args]
    scratch += [
        vm((n_tok, width), BF16),
        vm((half, width), BF16),
        vm((width, units), BF16),
        vm((width, units), BF16),
        vm((units, width), BF16),
        vm((2, groups, units), BF16),
        vm((2, ranks, 2, half // 2), F32),
        vm((15, 2, 2, half // 2), F32),
        vm((2, 2, half // 2), F32),
        vm((15, 2, 2, half // 2), F32),
        vm((2, 8, part, units), BF16),
        vm((half, units), F32),
        vm((2, 8, part, units), BF16),
        vm((7, 2, part, units), BF16),
        vm((2, 7, part, units), BF16),
        vm((2, 8, part, units), BF16),
        vm((2, 2, 4, share, width), F32),
        vm((2, 2, 4, share, width), BF16),
        vm((2, 3, 2, share, width), BF16),
        vm((2, 2, share, width), BF16),
        vm((4, share, width), BF16),
        pltpu.SemaphoreType.REGULAR,
    ]
    scratch += [
        dma(n)
        for n in (
            (10,), (5,), (5,), (15,), (15,), (15,), (15,),
            (7,), (7,), (2, 7), (2, 7), (2, 7), (2, 7), (2, 3), (2, 3), (2, 2), (4,),
        )
    ]
    any_spec = pl.BlockSpec(memory_space=pl.ANY)
    out = pl.pallas_call(
        kernel,
        out_shape=jax.ShapeDtypeStruct((share, width), BF16),
        in_specs=[any_spec] * len(args),
        out_specs=pl.BlockSpec(memory_space=pltpu.VMEM),
        scratch_shapes=scratch,
        compiler_params=pltpu.CompilerParams(
            collective_id=0, has_side_effects=True, vmem_limit_bytes=56 * 1024 * 1024
        ),
    )(*args)
    return out.reshape(share // draft, draft, width)


def solution(mesh):
    placed = (
        P(None, None, "row"),
        P(),
        P(),
        P(None, ("row", "col"), None),
        P(None, "row", "col"),
        P("row", "col"),
        P("row", "col"),
        P("col", "row"),
        P(),
        P(),
    )
    return jax.shard_map(
        shards, mesh=mesh, in_specs=placed, out_specs=P("col", None, "row"), check_vma=False
    )
```

```python
import functools

import jax
import jax.numpy as jnp
from jax import lax
from jax.experimental import pallas as pl
from jax.experimental.pallas import tpu as pltpu
from jax.sharding import PartitionSpec as P

MESH = pl.DeviceIdType.MESH
F32 = jnp.float32
BF16 = jnp.bfloat16


def dot(a, b, dims=((1,), (0,))):
    return lax.dot_general(a, b, (dims, ((), ())), preferred_element_type=F32)


def kernel(
    tokens, task_emb, gen_in, gen_a, gen_b, w_gate, w_up, w_down, count, task,
    out,
    tok3_v, emb_v, gin_v, ga_v, gb_v, wg_v, wu_v, wd_v, cnt_v, tsk_v,
    tok_v, tokp_v, wgp_v, wup_v, wdp_v, wdz_v, wdzp_v, b_v,
    low_s, low1_r, low2_s, low2_r,
    low_v, gate_s, gate_r, gate_f, gz_s, gz_r, up_f, up_s, up_r, hid_v, mix_f, mix_s, mix_r, end_s, end_r,
    known, load_sem, pair_ss, pair_rs, wz_ss, wz_rs, wf_ss, wf_rs, l1_ss, l1_rs, l2_ss, l2_rs,
    g_ss, g_rs, gz_ss, gz_rs, u_ss, u_rs, h_ss, h_rs, m_ss, m_rs, e_ss, e_rs,
):
    row = lax.axis_index("row")
    col = lax.axis_index("col")
    z_lo, y, core = row // 8, row // 2 % 4, row % 2
    z_hi, x = col // 4, col % 4
    chip = row // 2
    groups = count.shape[1]
    ranks = low_s.shape[1]
    mate = (row + 1 - 2 * core, col)
    zmate = ((row + 8) % 16, col)

    def in_row(dz, dy, dk, sign=1):
        return ((z_lo + dz) % 2 * 4 + (y + sign * dy + 4) % 4) * 2 + (core + dk) % 2

    def in_col(dz, dx):
        return (z_hi + dz) % 4 * 4 + (x + dx) % 4

    row_steps = [(dz, dy, dk) for dz in (1, 0) for dy in (2, 1, 3, 0) for dk in (1, 0)][:-1]
    col_steps = [(dz, dx) for dz in (2, 1, 3, 0) for dx in (2, 1, 3, 0)][:-1]
    y_steps = (2, 1, 3)
    chip_steps = [(dz, dy) for dz in (1, 0) for dy in (2, 1, 3, 0)][:-1]

    bar = pltpu.get_barrier_semaphore()
    for d in (2, 1, 3):
        pl.semaphore_signal(bar, inc=1, device_id=(row, in_col(d, 0)), device_id_type=MESH)
    for step in row_steps:
        pl.semaphore_signal(bar, inc=1, device_id=(in_row(*step), col), device_id_type=MESH)
    for d in (2, 1, 3):
        pl.semaphore_signal(bar, inc=1, device_id=(row, in_col(0, d)), device_id_type=MESH)

    loads = [
        pltpu.make_async_copy(src, dst, load_sem.at[n])
        for n, (src, dst) in enumerate(
            [
                (task, tsk_v), (task_emb, emb_v), (gen_in, gin_v), (count, cnt_v), (gen_a, ga_v),
                (tokens, tok3_v), (gen_b, gb_v), (w_gate, wg_v), (w_up, wu_v), (w_down, wd_v),
            ]
        )
    ]
    for c in loads:
        c.start()

    def copy(src, dst, ss, rs, dev):
        return pltpu.make_async_remote_copy(
            src_ref=src, dst_ref=dst, send_sem=ss, recv_sem=rs, device_id=dev, device_id_type=MESH
        )

    gi = lax.broadcasted_iota(jnp.int32, (groups, groups), 0)
    gj = lax.broadcasted_iota(jnp.int32, (groups, groups), 1)
    loads[0].wait()
    task_of = jnp.sum(jnp.where(gi == gj, tsk_v[...].astype(F32), 0.0), axis=1, keepdims=True)
    tasks = emb_v.shape[0]
    pick = lax.broadcasted_iota(jnp.int32, (groups, tasks), 1).astype(F32) == task_of
    loads[1].wait()
    chosen = dot(jnp.where(pick, 1.0, 0.0).astype(BF16), emb_v[...]).astype(BF16)
    loads[2].wait()
    hyper = jax.nn.silu(dot(chosen, gin_v[...])).astype(BF16)

    loads[3].wait()
    cnt = cnt_v[...].astype(F32)
    ends = jnp.sum(jnp.where(gj <= gi, cnt, 0.0), axis=1, keepdims=True)
    starts = ends - jnp.sum(jnp.where(gj == gi, cnt, 0.0), axis=1, keepdims=True)

    def member(first, width):
        request = (lax.broadcasted_iota(jnp.int32, (groups, width), 1) + first) // 2
        request = request.astype(F32)
        return jnp.where((request >= starts) & (request < ends), 1.0, 0.0)

    loads[4].wait()
    fac_a = dot(ga_v[...], hyper, ((1,), (1,))).astype(BF16)
    n_tok = tok_v.shape[0]
    width = tok_v.shape[1]
    slab = fac_a.shape[0] // ranks
    a_of = dot(fac_a, member(0, n_tok).astype(BF16))
    which = lax.broadcasted_iota(jnp.int32, (slab * ranks, width), 0) // ranks + col * slab
    sel = jnp.where(lax.broadcasted_iota(jnp.int32, (slab * ranks, width), 1) == which, 1.0, 0.0)
    loads[5].wait()
    tok_v[...] = tok3_v[...].reshape(n_tok, width)
    t_of = dot(sel.astype(BF16), tok_v[...], ((1,), (1,)))
    low = jnp.sum((a_of * t_of).reshape(slab, ranks, n_tok), axis=0)
    for h in range(2):
        for q in range(2):
            low_s[h, :, q, :] = low[:, h * 256 + q * 128 : h * 256 + q * 128 + 128]

    pl.semaphore_wait(bar, 21)
    for d in (2, 1, 3):
        pl.semaphore_signal(known, inc=1, device_id=(row, in_col(d, 0)), device_id_type=MESH)

    l1 = []
    for n, (dz, dy, dk) in enumerate(row_steps):
        to = in_row(dz, dy, dk)
        l1.append(
            copy(low_s.at[to % 2, pl.ds(to // 2 * 2, 2)], low1_r.at[n], l1_ss.at[n], l1_rs.at[n], (to, col))
        )
        l1[-1].start()
    half = tok_v.shape[0] // 2
    other = pl.ds(pl.multiple_of((1 - core) * half, half), half)
    mine = pl.ds(pl.multiple_of(core * half, half), half)
    for n in (7, 8, 9):
        loads[n].wait()
    pair = [
        copy(tok_v.at[other], tokp_v, pair_ss.at[0], pair_rs.at[0], mate),
        copy(wg_v, wgp_v, pair_ss.at[1], pair_rs.at[1], mate),
        copy(wu_v, wup_v, pair_ss.at[2], pair_rs.at[2], mate),
        copy(wd_v, wdp_v, pair_ss.at[3], pair_rs.at[3], mate),
        copy(b_v.at[core], b_v.at[core], pair_ss.at[4], pair_rs.at[4], mate),
    ]
    for n in range(2):
        pair[n].start()
    units = wd_v.shape[0]
    piece = units // 4
    wz = [
        copy(wd_v.at[pl.ds(n * piece, piece)], wdz_v.at[pl.ds(n * piece, piece)], wz_ss.at[n], wz_rs.at[n], zmate)
        for n in range(4)
    ]
    wf = [
        copy(
            wdz_v.at[pl.ds(n * 2 * piece, 2 * piece)], wdzp_v.at[pl.ds(n * 2 * piece, 2 * piece)],
            wf_ss.at[n], wf_rs.at[n], mate,
        )
        for n in range(2)
    ]
    wz[0].start()
    wz[1].start()
    pair[2].start()
    loads[6].wait()
    b_v[core] = dot(hyper, gb_v[...]).astype(BF16)
    pair[4].start()
    pair[3].start()

    gate = dot(tok_v[mine, :], wg_v[...])
    pair[0].wait_recv()
    pair[1].wait_recv()
    block = half // 2
    share = block // 4
    part = share // 2
    gate_s[...] = (gate + dot(tokp_v[...], wgp_v[...])).astype(BF16).reshape(2, 4, 2, part, units)
    gs = []
    for n, dy in enumerate(y_steps):
        to = (y + dy) % 4
        gs.append(copy(gate_s.at[:, to], gate_r.at[n], g_ss.at[n], g_rs.at[n], (in_row(0, dy, 0), col)))
        gs[-1].start()

    low = low_s[core, pl.ds(chip * 2, 2)]
    for n in range(15):
        l1[n].wait_recv()
        low = low + low1_r[n]
    low2_s[...] = low
    pl.semaphore_wait(known, 3)
    l2 = []
    for n, (dz, dx) in enumerate(col_steps):
        l2.append(copy(low2_s, low2_r.at[n], l2_ss.at[n], l2_rs.at[n], (row, in_col(dz, dx))))
        l2[-1].start()
    wz[2].start()
    wz[3].start()

    up = dot(tok_v[mine, :], wu_v[...])
    pair[2].wait_recv()
    up_f[...] = up + dot(tokp_v[...], wup_v[...])
    pair[4].wait_recv()
    wz[0].wait_recv()
    wz[1].wait_recv()
    wf[0].start()
    for c in gs:
        c.wait_recv()

    def gate_sum(q):
        total = gate_s[q, y].astype(F32)
        for n in range(3):
            total = total + gate_r[n, q].astype(F32)
        return total

    gz_s[...] = gate_sum(1 - z_lo).astype(BF16)
    gz = copy(gz_s, gz_r, gz_ss, gz_rs, zmate)
    gz.start()
    gate_f[...] = gate_sum(z_lo)

    b_all = b_v[...].reshape(2 * groups, units)
    quarters = (1 - z_lo, z_lo)
    mem = [member(core * half + q * block, block) for q in quarters]
    for n in range(15):
        l2[n].wait_recv()
        low = low + low2_r[n]
    low_v[...] = low.astype(BF16).astype(F32)
    us = [[None] * 7 for _ in range(2)]

    def send_up(a, across):
        for n, (dz, dy) in enumerate(chip_steps):
            if dz == across:
                src = up_s.at[(z_lo + dz) % 2, (y + dy) % 4, a]
                to = (in_row(dz, dy, 0), col)
                us[a][n] = copy(src, up_r.at[a, n], u_ss.at[a, n], u_rs.at[a, n], to)
                us[a][n].start()

    for t, q in enumerate(quarters):
        spread = jnp.concatenate([mem[t] * low_v[r, pl.ds(q, 1), :] for r in range(2)], axis=0).astype(BF16)
        here = pl.ds(pl.multiple_of(q * block, block), block)
        up = up_f[here, :] + dot(spread, b_all, ((0,), (0,)))
        up_s[q] = up.astype(BF16).reshape(4, 2, part, units)
        send_up(0, 1 - t)
    send_up(1, 1)
    send_up(1, 0)
    wz[2].wait_recv()
    wz[3].wait_recv()
    wf[1].start()

    gz.wait_recv()
    hs = []
    for a in range(2):
        act = jax.nn.silu(gate_f[a] + gz_r[a].astype(F32))
        up = up_s[z_lo, y, a].astype(F32)
        for n in range(7):
            us[a][n].wait_recv()
            up = up + up_r[a, n].astype(F32)
        hid_v[a, y] = (act * up).astype(BF16)
        hs.append([])
        for n, dy in enumerate(y_steps):
            hs[a].append(
                copy(hid_v.at[a, y], hid_v.at[a, y], h_ss.at[a, n], h_rs.at[a, n], (in_row(0, dy, 0), col))
            )
            hs[a][-1].start()

    pair[3].wait_recv()
    for c in wf:
        c.wait_recv()
    ms = []
    for a in range(2):
        for n, dy in enumerate(y_steps):
            src = (y + 4 - dy) % 4
            copy(hid_v.at[a, src], hid_v.at[a, src], h_ss.at[a, n], h_rs.at[a, n], (row, col)).wait_recv()
        hid = hid_v[a].reshape(4 * part, units)
        for k, w in enumerate((wd_v, wdp_v, wdz_v, wdzp_v)):
            mix = dot(hid, w[...]).reshape(4, part, width)
            mix_f[a, k] = mix
            mix_s[a, k] = mix.astype(BF16)
        ms.append([])
        for n, d in enumerate((2, 1, 3)):
            ms[a].append(
                copy(mix_s.at[a, :, (x + d) % 4], mix_r.at[a, n], m_ss.at[a, n], m_rs.at[a, n], (row, in_col(0, d)))
            )
            ms[a][-1].start()
    es = []
    to = (2 * core + z_lo) * 4 + x
    stays = z_hi == 2 * core + z_lo
    for a in range(2):
        mix = mix_f[a, :, x]
        for n in range(3):
            ms[a][n].wait_recv()
            mix = mix + mix_r[a, n].astype(F32)
        end_s[a] = mix.astype(BF16)
        for k, dev in enumerate((row, mate[0], zmate[0], in_row(1, 0, 1))):
            c = copy(end_s.at[a, k], end_r.at[a, z_hi], e_ss.at[a, k], e_rs.at[a, z_hi], (dev, to))
            if k == 0:
                pl.when(jnp.logical_not(stays))(c.start)
            else:
                c.start()
            es.append((k == 0, c))

        @pl.when(stays)
        def _():
            end_r[a, z_hi] = end_s[a, 0]

    for a in range(2):
        for s in range(4):
            arrived = copy(end_r.at[a, s], end_r.at[a, s], e_ss.at[0, 0], e_rs.at[a, s], (row, col))
            pl.when(jnp.logical_not(stays & (z_hi == s)))(arrived.wait_recv)
        total = end_r[a, 0].astype(F32)
        for s in range(1, 4):
            total = total + end_r[a, s].astype(F32)
        out[pl.ds(a * part, part), :] = total.astype(BF16)

    for c in l1 + l2 + pair + wz + wf + gs + [gz] + us[0] + us[1] + hs[0] + hs[1] + ms[0] + ms[1]:
        c.wait_send()
    for local, c in es:
        if local:
            pl.when(jnp.logical_not(stays))(c.wait_send)
        else:
            c.wait_send()


def shards(tokens, task_emb, gen_in, gen_a, gen_b, w_gate, w_up, w_down, group_count, group_task):
    batch, draft, width = tokens.shape
    hyper, slab, ranks = gen_a.shape
    groups = group_count.shape[0]
    units = w_gate.shape[1]
    n_tok = batch * draft
    half = n_tok // 2
    share = half // 8
    part = share // 2
    vm = pltpu.VMEM
    dma = pltpu.SemaphoreType.DMA
    args = (
        tokens,
        task_emb,
        gen_in,
        gen_a.transpose(1, 2, 0).reshape(slab * ranks, hyper),
        gen_b.reshape(hyper, units),
        w_gate,
        w_up,
        w_down,
        group_count.reshape(1, groups),
        group_task.reshape(1, groups),
    )
    scratch = [vm(a.shape, a.dtype) for a in args]
    scratch += [
        vm((n_tok, width), BF16),
        vm((half, width), BF16),
        vm((width, units), BF16),
        vm((width, units), BF16),
        vm((units, width), BF16),
        vm((units, width), BF16),
        vm((units, width), BF16),
        vm((2, groups, units), BF16),
        vm((2, ranks, 2, half // 2), F32),
        vm((15, 2, 2, half // 2), F32),
        vm((2, 2, half // 2), F32),
        vm((15, 2, 2, half // 2), F32),
        vm((2, 2, half // 2), F32),
        vm((2, 4, 2, part, units), BF16),
        vm((3, 2, 2, part, units), BF16),
        vm((2, part, units), F32),
        vm((2, part, units), BF16),
        vm((2, part, units), BF16),
        vm((half, units), F32),
        vm((2, 4, 2, part, units), BF16),
        vm((2, 7, part, units), BF16),
        vm((2, 4, part, units), BF16),
        vm((2, 4, 4, part, width), F32),
        vm((2, 4, 4, part, width), BF16),
        vm((2, 3, 4, part, width), BF16),
        vm((2, 4, part, width), BF16),
        vm((2, 4, part, width), BF16),
        pltpu.SemaphoreType.REGULAR,
        dma((10,)),
        dma((5,)),
        dma((5,)),
        dma((4,)),
        dma((4,)),
        dma((2,)),
        dma((2,)),
        dma((15,)),
        dma((15,)),
        dma((15,)),
        dma((15,)),
        dma((3,)),
        dma((3,)),
        dma,
        dma,
        dma((2, 7)),
        dma((2, 7)),
        dma((2, 3)),
        dma((2, 3)),
        dma((2, 3)),
        dma((2, 3)),
        dma((2, 4)),
        dma((2, 4)),
    ]
    any_spec = pl.BlockSpec(memory_space=pl.ANY)
    out = pl.pallas_call(
        kernel,
        out_shape=jax.ShapeDtypeStruct((share, width), BF16),
        in_specs=[any_spec] * len(args),
        out_specs=pl.BlockSpec(memory_space=pltpu.VMEM),
        scratch_shapes=scratch,
        compiler_params=pltpu.CompilerParams(
            collective_id=0, has_side_effects=True, vmem_limit_bytes=32 * 1024 * 1024
        ),
    )(*[pltpu.with_memory_space_constraint(a, pltpu.HBM) for a in args])
    return out.reshape(share // draft, draft, width)


def solution(mesh):
    placed = (
        P(None, None, "row"),
        P(),
        P(),
        P(None, ("row", "col"), None),
        P(None, "row", "col"),
        P("row", "col"),
        P("row", "col"),
        P("col", "row"),
        P(),
        P(),
    )
    return jax.shard_map(
        shards, mesh=mesh, in_specs=placed, out_specs=P("col", None, "row"), check_vma=False
    )
```

```python
import functools

import jax
import jax.numpy as jnp
from jax import lax
from jax.experimental import pallas as pl
from jax.experimental.pallas import tpu as pltpu
from jax.sharding import PartitionSpec as P

MESH = pl.DeviceIdType.MESH
F32 = jnp.float32
BF16 = jnp.bfloat16


def dot(a, b, dims=((1,), (0,))):
    return lax.dot_general(a, b, (dims, ((), ())), preferred_element_type=F32)


def kernel(
    tokens, task_emb, gen_in, gen_a, gen_b, w_gate, w_up, w_down, count, task,
    out,
    tok3_v, emb_v, gin_v, ga_v, gb_v, wg_v, wu_v, wd_v, cnt_v, tsk_v,
    tok_v, tokp_v, wgp_v, wup_v, wdp_v, b_v,
    low_s, low1_r, low2_s, low2_r,
    gate_s, up_f, up_s, gate_r, up_r, hid_v, mix_f, mix_s, mix_r, end_s, end_r,
    known, load_sem, pair_ss, pair_rs, l1_ss, l1_rs, l2_ss, l2_rs,
    g_ss, g_rs, u_ss, u_rs, h_ss, h_rs, m_ss, m_rs, e_ss, e_rs,
):
    row = lax.axis_index("row")
    col = lax.axis_index("col")
    z_lo, y, core = row // 8, row // 2 % 4, row % 2
    z_hi, x = col // 4, col % 4
    chip = row // 2
    groups = count.shape[1]
    ranks = low_s.shape[1]
    mate = (row + 1 - 2 * core, col)

    def in_row(dz, dy, dk, sign=1):
        return ((z_lo + dz) % 2 * 4 + (y + sign * dy + 4) % 4) * 2 + (core + dk) % 2

    def in_col(dz, dx):
        return (z_hi + dz) % 4 * 4 + (x + dx) % 4

    row_steps = [(dz, dy, dk) for dz in (1, 0) for dy in (2, 1, 3, 0) for dk in (1, 0)][:-1]
    col_steps = [(dz, dx) for dz in (2, 1, 3, 0) for dx in (2, 1, 3, 0)][:-1]
    chip_steps = [(dz, dy) for dz in (1, 0) for dy in (2, 1, 3, 0)][:-1]

    bar = pltpu.get_barrier_semaphore()
    for d in (2, 1, 3):
        pl.semaphore_signal(bar, inc=1, device_id=(row, in_col(d, 0)), device_id_type=MESH)
    for step in row_steps:
        pl.semaphore_signal(bar, inc=1, device_id=(in_row(*step), col), device_id_type=MESH)
    for d in (2, 1, 3):
        pl.semaphore_signal(bar, inc=1, device_id=(row, in_col(0, d)), device_id_type=MESH)

    loads = [
        pltpu.make_async_copy(src, dst, load_sem.at[n])
        for n, (src, dst) in enumerate(
            [
                (task, tsk_v), (task_emb, emb_v), (gen_in, gin_v), (count, cnt_v), (gen_a, ga_v),
                (tokens, tok3_v), (gen_b, gb_v), (w_gate, wg_v), (w_up, wu_v), (w_down, wd_v),
            ]
        )
    ]
    for c in loads:
        c.start()

    def copy(src, dst, ss, rs, dev):
        return pltpu.make_async_remote_copy(
            src_ref=src, dst_ref=dst, send_sem=ss, recv_sem=rs, device_id=dev, device_id_type=MESH
        )

    gi = lax.broadcasted_iota(jnp.int32, (groups, groups), 0)
    gj = lax.broadcasted_iota(jnp.int32, (groups, groups), 1)
    loads[0].wait()
    task_of = jnp.sum(jnp.where(gi == gj, tsk_v[...].astype(F32), 0.0), axis=1, keepdims=True)
    tasks = emb_v.shape[0]
    pick = lax.broadcasted_iota(jnp.int32, (groups, tasks), 1).astype(F32) == task_of
    loads[1].wait()
    chosen = dot(jnp.where(pick, 1.0, 0.0).astype(BF16), emb_v[...]).astype(BF16)
    loads[2].wait()
    hyper = jax.nn.silu(dot(chosen, gin_v[...])).astype(BF16)

    loads[3].wait()
    cnt = cnt_v[...].astype(F32)
    ends = jnp.sum(jnp.where(gj <= gi, cnt, 0.0), axis=1, keepdims=True)
    starts = ends - jnp.sum(jnp.where(gj == gi, cnt, 0.0), axis=1, keepdims=True)

    def member(first, width):
        request = (lax.broadcasted_iota(jnp.int32, (groups, width), 1) + first) // 2
        request = request.astype(F32)
        return jnp.where((request >= starts) & (request < ends), 1.0, 0.0)

    loads[4].wait()
    fac_a = dot(ga_v[...], hyper, ((1,), (1,))).astype(BF16)
    n_tok = tok_v.shape[0]
    width = tok_v.shape[1]
    slab = fac_a.shape[0] // ranks
    a_of = dot(fac_a, member(0, n_tok).astype(BF16))
    which = lax.broadcasted_iota(jnp.int32, (slab * ranks, width), 0) // ranks + col * slab
    sel = jnp.where(lax.broadcasted_iota(jnp.int32, (slab * ranks, width), 1) == which, 1.0, 0.0)
    loads[5].wait()
    tok_v[...] = tok3_v[...].reshape(n_tok, width)
    t_of = dot(sel.astype(BF16), tok_v[...], ((1,), (1,)))
    low = jnp.sum((a_of * t_of).reshape(slab, ranks, n_tok), axis=0)
    for h in range(2):
        for q in range(2):
            low_s[h, :, q, :] = low[:, h * 256 + q * 128 : h * 256 + q * 128 + 128]

    pl.semaphore_wait(bar, 21)
    for d in (2, 1, 3):
        pl.semaphore_signal(known, inc=1, device_id=(row, in_col(d, 0)), device_id_type=MESH)

    l1 = []
    for n, (dz, dy, dk) in enumerate(row_steps):
        to = in_row(dz, dy, dk)
        l1.append(
            copy(low_s.at[to % 2, pl.ds(to // 2 * 2, 2)], low1_r.at[n], l1_ss.at[n], l1_rs.at[n], (to, col))
        )
        l1[-1].start()
    half = tok_v.shape[0] // 2
    other = pl.ds(pl.multiple_of((1 - core) * half, half), half)
    mine = pl.ds(pl.multiple_of(core * half, half), half)
    for n in (7, 8, 9):
        loads[n].wait()
    pair = [
        copy(tok_v.at[other], tokp_v, pair_ss.at[0], pair_rs.at[0], mate),
        copy(wg_v, wgp_v, pair_ss.at[1], pair_rs.at[1], mate),
        copy(wu_v, wup_v, pair_ss.at[2], pair_rs.at[2], mate),
        copy(wd_v, wdp_v, pair_ss.at[3], pair_rs.at[3], mate),
        copy(b_v.at[core], b_v.at[core], pair_ss.at[4], pair_rs.at[4], mate),
    ]
    for n in range(4):
        pair[n].start()
    loads[6].wait()
    b_v[core] = dot(hyper, gb_v[...]).astype(BF16)
    pair[4].start()

    gate = dot(tok_v[mine, :], wg_v[...])
    pair[0].wait_recv()
    pair[1].wait_recv()
    share = half // 8
    part = share // 2
    units = gate.shape[1]
    gate_s[...] = (gate + dot(tokp_v[...], wgp_v[...])).astype(BF16).reshape(2, 8, part, units)

    def peer(dz, dy, sign=1):
        return in_row(dz, dy, 0, sign) // 2

    gs = []
    for n, (dz, dy) in enumerate(chip_steps):
        i = peer(dz, dy)
        gs.append(copy(gate_s.at[:, i], gate_r.at[n], g_ss.at[n], g_rs.at[n], (i * 2 + core, col)))
    for n, (dz, dy) in enumerate(chip_steps):
        if dz == 0:
            gs[n].start()

    low = low_s[core, pl.ds(chip * 2, 2)]
    for n in range(15):
        l1[n].wait_recv()
        low = low + low1_r[n]
    low2_s[...] = low
    pl.semaphore_wait(known, 3)
    l2 = []
    for n, (dz, dx) in enumerate(col_steps):
        l2.append(copy(low2_s, low2_r.at[n], l2_ss.at[n], l2_rs.at[n], (row, in_col(dz, dx))))
        l2[-1].start()
    for n, (dz, dy) in enumerate(chip_steps):
        if dz == 1:
            gs[n].start()

    up = dot(tok_v[mine, :], wu_v[...])
    pair[2].wait_recv()
    up_f[...] = up + dot(tokp_v[...], wup_v[...])
    pair[4].wait_recv()
    b_all = b_v[...].reshape(2 * groups, units)
    block = half // 2
    mem = [member(core * half + a * block, block) for a in range(2)]
    for n in range(15):
        l2[n].wait_recv()
        low = low + low2_r[n]
    low = low.astype(BF16).astype(F32)
    us = []
    for a in range(2):
        spread = jnp.concatenate([mem[a] * low[r, a : a + 1, :] for r in range(2)], axis=0).astype(BF16)
        up = up_f[a * block : a * block + block, :] + dot(spread, b_all, ((0,), (0,)))
        up_s[a] = up.astype(BF16).reshape(8, part, units)
        us.append([])
        for n, (dz, dy) in enumerate(chip_steps):
            i = peer(dz, dy)
            us[a].append(
                copy(up_s.at[a, i], up_r.at[a, n], u_ss.at[a, n], u_rs.at[a, n], (i * 2 + core, col))
            )
            us[a][-1].start()

    for n in range(7):
        gs[n].wait_recv()
    hs = []
    for a in range(2):
        gate = gate_s[a, chip].astype(F32)
        for n in range(7):
            gate = gate + gate_r[n, a].astype(F32)
        act = jax.nn.silu(gate)
        up = up_s[a, chip].astype(F32)
        for n in range(7):
            us[a][n].wait_recv()
            up = up + up_r[a, n].astype(F32)
        hid_v[a, chip] = (act * up).astype(BF16)
        hs.append([])
        for n, (dz, dy) in enumerate(chip_steps):
            hs[a].append(
                copy(
                    hid_v.at[a, chip], hid_v.at[a, chip], h_ss.at[a, n], h_rs.at[a, n],
                    (peer(dz, dy) * 2 + core, col),
                )
            )
            hs[a][-1].start()

    pair[3].wait_recv()
    ms = []
    for a in range(2):
        for n, (dz, dy) in enumerate(chip_steps):
            src = peer(dz, dy, -1)
            copy(hid_v.at[a, src], hid_v.at[a, src], h_ss.at[a, n], h_rs.at[a, n], (row, col)).wait_recv()
        hid = hid_v[a].reshape(block, units)
        for k, w in enumerate((wd_v, wdp_v)):
            mix = dot(hid, w[...])
            mix_f[a, k] = mix.reshape(4, share, width)
            mix_s[a, k] = mix.astype(BF16).reshape(4, share, width)
        ms.append([])
        for n, d in enumerate((2, 1, 3)):
            ms[a].append(
                copy(mix_s.at[a, :, (x + d) % 4], mix_r.at[a, n], m_ss.at[a, n], m_rs.at[a, n], (row, in_col(0, d)))
            )
            ms[a][-1].start()
    es = []
    for a in range(2):
        to = 2 * core + a
        here = z_hi == to
        mix = mix_f[a, :, x]
        for n in range(3):
            ms[a][n].wait_recv()
            mix = mix + mix_r[a, n].astype(F32)
        end_s[a] = mix.astype(BF16)
        cross = copy(end_s.at[a, 1], end_r.at[z_hi], e_ss.at[a, 1], e_rs.at[z_hi], (mate[0], to * 4 + x))
        same = copy(end_s.at[a, 0], end_r.at[z_hi], e_ss.at[a, 0], e_rs.at[z_hi], (row, to * 4 + x))
        pl.when(jnp.logical_not(here))(same.start)
        cross.start()

        @pl.when(here)
        def _():
            end_r[z_hi] = end_s[a, 0]

        es.append((same, cross, here))

    mine = z_hi // 2 == core
    for s in range(4):
        arrived = copy(end_r.at[s], end_r.at[s], e_ss.at[0, 0], e_rs.at[s], (row, col))
        pl.when(jnp.logical_not(mine & (z_hi == s)))(arrived.wait_recv)
    total = end_r[0].astype(F32)
    for s in range(1, 4):
        total = total + end_r[s].astype(F32)
    out[...] = total.astype(BF16)

    for c in l1 + l2 + pair + gs + us[0] + us[1] + hs[0] + hs[1] + ms[0] + ms[1]:
        c.wait_send()
    for same, cross, here in es:
        pl.when(jnp.logical_not(here))(same.wait_send)
        cross.wait_send()


def shards(tokens, task_emb, gen_in, gen_a, gen_b, w_gate, w_up, w_down, group_count, group_task):
    batch, draft, width = tokens.shape
    hyper, slab, ranks = gen_a.shape
    groups = group_count.shape[0]
    units = w_gate.shape[1]
    n_tok = batch * draft
    half = n_tok // 2
    share = half // 8
    part = share // 2
    vm = pltpu.VMEM
    dma = pltpu.SemaphoreType.DMA
    args = (
        tokens,
        task_emb,
        gen_in,
        gen_a.transpose(1, 2, 0).reshape(slab * ranks, hyper),
        gen_b.reshape(hyper, units),
        w_gate,
        w_up,
        w_down,
        group_count.reshape(1, groups),
        group_task.reshape(1, groups),
    )
    scratch = [vm(a.shape, a.dtype) for a in args]
    scratch += [
        vm((n_tok, width), BF16),
        vm((half, width), BF16),
        vm((width, units), BF16),
        vm((width, units), BF16),
        vm((units, width), BF16),
        vm((2, groups, units), BF16),
        vm((2, ranks, 2, half // 2), F32),
        vm((15, 2, 2, half // 2), F32),
        vm((2, 2, half // 2), F32),
        vm((15, 2, 2, half // 2), F32),
        vm((2, 8, part, units), BF16),
        vm((half, units), F32),
        vm((2, 8, part, units), BF16),
        vm((7, 2, part, units), BF16),
        vm((2, 7, part, units), BF16),
        vm((2, 8, part, units), BF16),
        vm((2, 2, 4, share, width), F32),
        vm((2, 2, 4, share, width), BF16),
        vm((2, 3, 2, share, width), BF16),
        vm((2, 2, share, width), BF16),
        vm((4, share, width), BF16),
        pltpu.SemaphoreType.REGULAR,
    ]
    scratch += [
        dma(n)
        for n in (
            (10,), (5,), (5,), (15,), (15,), (15,), (15,),
            (7,), (7,), (2, 7), (2, 7), (2, 7), (2, 7), (2, 3), (2, 3), (2, 2), (4,),
        )
    ]
    any_spec = pl.BlockSpec(memory_space=pl.ANY)
    out = pl.pallas_call(
        kernel,
        out_shape=jax.ShapeDtypeStruct((share, width), BF16),
        in_specs=[any_spec] * len(args),
        out_specs=pl.BlockSpec(memory_space=pltpu.VMEM),
        scratch_shapes=scratch,
        compiler_params=pltpu.CompilerParams(
            collective_id=0, has_side_effects=True, vmem_limit_bytes=32 * 1024 * 1024
        ),
    )(*[pltpu.with_memory_space_constraint(a, pltpu.HBM) for a in args])
    return out.reshape(share // draft, draft, width)


def solution(mesh):
    placed = (
        P(None, None, "row"),
        P(),
        P(),
        P(None, ("row", "col"), None),
        P(None, "row", "col"),
        P("row", "col"),
        P("row", "col"),
        P("col", "row"),
        P(),
        P(),
    )
    return jax.shard_map(
        shards, mesh=mesh, in_specs=placed, out_specs=P("col", None, "row"), check_vma=False
    )
```

```python
import functools

import jax
import jax.numpy as jnp
from jax import lax
from jax.experimental import pallas as pl
from jax.experimental.pallas import tpu as pltpu
from jax.sharding import PartitionSpec as P

MESH = pl.DeviceIdType.MESH
F32 = jnp.float32
BF16 = jnp.bfloat16


def dot(a, b, dims=((1,), (0,))):
    return lax.dot_general(a, b, (dims, ((), ())), preferred_element_type=F32)


def kernel(
    tokens, task_emb, gen_in, gen_a, gen_b, w_gate, w_up, w_down, count, task,
    out,
    tok3_v, emb_v, gin_v, ga_v, gb_v, wg_v, wu_v, wd_v, cnt_v, tsk_v,
    tok_v, tokp_v, wgp_v, wup_v, wdp_v, bs_s, bs_r,
    low_s, low1_r, low2_s, low2_r,
    gate_s, up_s, gate_r, up_r, hid_v, mix_f, mix_s, mix_r, end_s, end_r,
    known, load_sem, pair_ss, pair_rs, l1_ss, l1_rs, l2_ss, l2_rs, b_ss, b_rs,
    g_ss, g_rs, u_ss, u_rs, h_ss, h_rs, m_ss, m_rs, e_ss, e_rs,
):
    row = lax.axis_index("row")
    col = lax.axis_index("col")
    z_lo, y, core = row // 8, row // 2 % 4, row % 2
    z_hi, x = col // 4, col % 4
    chip = row // 2
    groups = count.shape[1]
    ranks = bs_r.shape[0]
    mate = (row + 1 - 2 * core, col)

    def in_row(dz, dy, dk, sign=1):
        return ((z_lo + dz) % 2 * 4 + (y + sign * dy + 4) % 4) * 2 + (core + dk) % 2

    def in_col(dz, dx):
        return (z_hi + dz) % 4 * 4 + (x + dx) % 4

    row_steps = [(dz, dy, dk) for dz in (1, 0) for dy in (2, 1, 3, 0) for dk in (1, 0)][:-1]
    col_steps = [(dz, dx) for dz in (2, 1, 3, 0) for dx in (2, 1, 3, 0)][:-1]
    chip_steps = [(dz, dy) for dz in (1, 0) for dy in (2, 1, 3, 0)][:-1]

    bar = pltpu.get_barrier_semaphore()
    for d in (2, 1, 3):
        pl.semaphore_signal(bar, inc=1, device_id=(row, in_col(d, 0)), device_id_type=MESH)
    for step in row_steps:
        pl.semaphore_signal(bar, inc=1, device_id=(in_row(*step), col), device_id_type=MESH)
    for d in (2, 1, 3):
        pl.semaphore_signal(bar, inc=1, device_id=(row, in_col(0, d)), device_id_type=MESH)

    loads = [
        pltpu.make_async_copy(src, dst, load_sem.at[n])
        for n, (src, dst) in enumerate(
            [
                (task, tsk_v), (task_emb, emb_v), (gen_in, gin_v), (count, cnt_v), (gen_b, gb_v), (gen_a, ga_v),
                (tokens, tok3_v), (w_gate, wg_v), (w_up, wu_v), (w_down, wd_v),
            ]
        )
    ]
    for c in loads:
        c.start()

    def copy(src, dst, ss, rs, dev):
        return pltpu.make_async_remote_copy(
            src_ref=src, dst_ref=dst, send_sem=ss, recv_sem=rs, device_id=dev, device_id_type=MESH
        )

    gi = lax.broadcasted_iota(jnp.int32, (groups, groups), 0)
    gj = lax.broadcasted_iota(jnp.int32, (groups, groups), 1)
    loads[0].wait()
    task_of = jnp.sum(jnp.where(gi == gj, tsk_v[...].astype(F32), 0.0), axis=1, keepdims=True)
    tasks = emb_v.shape[0]
    pick = lax.broadcasted_iota(jnp.int32, (groups, tasks), 1).astype(F32) == task_of
    loads[1].wait()
    chosen = dot(jnp.where(pick, 1.0, 0.0).astype(BF16), emb_v[...]).astype(BF16)
    loads[2].wait()
    hyper = jax.nn.silu(dot(chosen, gin_v[...])).astype(BF16)

    loads[3].wait()
    cnt = cnt_v[...].astype(F32)
    cnt_of = jnp.sum(jnp.where(gi == gj, cnt, 0.0), axis=1, keepdims=True)
    ends = jnp.sum(jnp.where(gj <= gi, cnt, 0.0), axis=1, keepdims=True)
    starts = ends - cnt_of
    ends_t = jnp.sum(jnp.where(gi <= gj, cnt_of, 0.0), axis=0, keepdims=True)
    starts_t = ends_t - cnt

    n_tok = tok_v.shape[0]
    width = tok_v.shape[1]
    half = n_tok // 2
    units = wd_v.shape[0]
    block = half // 2
    share = half // 8
    part = share // 2
    drafts = 2
    own = part // drafts

    def iota(rows, cols, dim):
        return lax.broadcasted_iota(jnp.int32, (rows, cols), dim)

    m = iota(groups, n_tok // drafts, 1)
    request = m // 128 * 128 + m // own % 2 * 64 + m // (2 * own) % 8 * own + m % own
    request = request.astype(F32)
    member = jnp.where((request >= starts) & (request < ends), 1.0, 0.0).astype(BF16)
    loads[4].wait()
    fac_b = dot(hyper, gb_v[...]).astype(BF16)
    bs_s[...] = dot(member, fac_b, ((0,), (0,))).astype(BF16).reshape(2, 8, 2 * own, units)

    loads[5].wait()
    fac_a = dot(hyper, ga_v[...], ((1,), (1,))).astype(BF16)
    cols = fac_a.shape[1]
    request = (iota(n_tok, groups, 0) // drafts).astype(F32)
    member = jnp.where((request >= starts_t) & (request < ends_t), 1.0, 0.0).astype(BF16)
    a_of = dot(member, fac_a)
    sel = iota(width, cols, 0) == iota(width, cols, 1) // ranks + col * (cols // ranks)
    loads[6].wait()
    tok_v[...] = tok3_v[...].reshape(n_tok, width)
    prod = a_of * dot(tok_v[...], jnp.where(sel, 1.0, 0.0).astype(BF16))
    high = prod.astype(BF16)
    rest = (prod - high.astype(F32)).astype(BF16)
    lanes = ranks * 2 * own
    place = jnp.where(iota(cols, lanes, 0) % ranks == iota(cols, lanes, 1) // (2 * own), 1.0, 0.0).astype(BF16)
    t = iota(n_tok, lanes, 0)
    at = t // block % 2 * own + t // drafts % own
    spread = jnp.where(at == iota(n_tok, lanes, 1) % (2 * own), dot(high, place) + dot(rest, place), 0.0)
    t = iota(32, n_tok, 1)
    to_row = t // half * 16 + t // part % 8 * drafts + t % drafts == iota(32, n_tok, 0)
    low = lax.dot_general(
        jnp.where(to_row, 1.0, 0.0), spread, (((1,), (0,)), ((), ())),
        precision=lax.Precision.HIGHEST, preferred_element_type=F32,
    )
    for h in range(2):
        for i in range(8):
            low_s[h, i] = low[h * 16 + i * 2 : h * 16 + i * 2 + 2, :]

    pl.semaphore_wait(bar, 21)
    for d in (2, 1, 3):
        pl.semaphore_signal(known, inc=1, device_id=(row, in_col(d, 0)), device_id_type=MESH)

    l1 = []
    for n, (dz, dy, dk) in enumerate(row_steps):
        to = in_row(dz, dy, dk)
        l1.append(copy(low_s.at[to % 2, to // 2], low1_r.at[n], l1_ss.at[n], l1_rs.at[n], (to, col)))
        l1[-1].start()
    other = pl.ds(pl.multiple_of((1 - core) * half, half), half)
    mine = pl.ds(pl.multiple_of(core * half, half), half)
    for n in (7, 8, 9):
        loads[n].wait()
    pair = [
        copy(tok_v.at[other], tokp_v, pair_ss.at[0], pair_rs.at[0], mate),
        copy(wg_v, wgp_v, pair_ss.at[1], pair_rs.at[1], mate),
        copy(wu_v, wup_v, pair_ss.at[2], pair_rs.at[2], mate),
        copy(wd_v, wdp_v, pair_ss.at[3], pair_rs.at[3], mate),
    ]
    for c in pair[:3]:
        c.start()
    bs = []
    for n, (dz, dy, dk) in enumerate(row_steps):
        to = in_row(dz, dy, dk)
        bs.append(copy(bs_s.at[to % 2, to // 2], bs_r.at[row], b_ss.at[n], b_rs.at[row], (to, col)))
        bs[-1].start()
    pair[3].start()
    bs_r[row] = bs_s[core, chip]

    gate = dot(tok_v[mine, :], wg_v[...])
    pair[0].wait_recv()
    pair[1].wait_recv()
    gate_s[...] = (gate + dot(tokp_v[...], wgp_v[...])).astype(BF16).reshape(2, 8, part, units)

    def peer(dz, dy, sign=1):
        return in_row(dz, dy, 0, sign) // 2

    gs = []
    for n, (dz, dy) in enumerate(chip_steps):
        i = peer(dz, dy)
        gs.append(copy(gate_s.at[:, i], gate_r.at[n], g_ss.at[n], g_rs.at[n], (i * 2 + core, col)))
    for n, (dz, dy) in enumerate(chip_steps):
        if dz == 0:
            gs[n].start()
    up = dot(tok_v[mine, :], wu_v[...])
    pair[2].wait_recv()
    up_s[...] = (up + dot(tokp_v[...], wup_v[...])).astype(BF16).reshape(2, 8, part, units)

    low = low_s[core, chip]
    for n in range(15):
        l1[n].wait_recv()
        low = low + low1_r[n]
    low2_s[...] = low
    pl.semaphore_wait(known, 3)
    l2 = []
    for n, (dz, dx) in enumerate(col_steps):
        l2.append(copy(low2_s, low2_r.at[n], l2_ss.at[n], l2_rs.at[n], (row, in_col(dz, dx))))
        l2[-1].start()
    for n, (dz, dy) in enumerate(chip_steps):
        if dz == 1:
            gs[n].start()
    us = []
    for a in range(2):
        us.append([])
        for n, (dz, dy) in enumerate(chip_steps):
            i = peer(dz, dy)
            us[a].append(
                copy(up_s.at[a, i], up_r.at[a, n], u_ss.at[a, n], u_rs.at[a, n], (i * 2 + core, col))
            )
            us[a][-1].start()

    for n in range(15):
        l2[n].wait_recv()
        low = low + low2_r[n]
    low = low.astype(BF16).astype(F32)
    m = iota(share, lanes, 0)
    low = jnp.where(m % 2 == 0, low[0:1, :], low[1:2, :])
    low = jnp.where(m // drafts == iota(share, lanes, 1) % (2 * own), low, 0.0).astype(BF16)
    for n, (dz, dy, dk) in enumerate(row_steps):
        src = in_row(dz, dy, dk, -1)
        copy(bs_s.at[0, 0], bs_r.at[src], b_ss.at[n], b_rs.at[src], (row, col)).wait_recv()
    lora = dot(low, bs_r[...].reshape(lanes, units))

    for n in range(7):
        gs[n].wait_recv()
    hs = []
    for a in range(2):
        gate = gate_s[a, chip].astype(F32)
        for n in range(7):
            gate = gate + gate_r[n, a].astype(F32)
        act = jax.nn.silu(gate)
        up = up_s[a, chip].astype(F32) + lora[a * part : a * part + part, :]
        for n in range(7):
            us[a][n].wait_recv()
            up = up + up_r[a, n].astype(F32)
        hid_v[a, chip] = (act * up).astype(BF16)
        hs.append([])
        for n, (dz, dy) in enumerate(chip_steps):
            hs[a].append(
                copy(
                    hid_v.at[a, chip], hid_v.at[a, chip], h_ss.at[a, n], h_rs.at[a, n],
                    (peer(dz, dy) * 2 + core, col),
                )
            )
            hs[a][-1].start()

    pair[3].wait_recv()
    ms = []
    for a in range(2):
        for n, (dz, dy) in enumerate(chip_steps):
            src = peer(dz, dy, -1)
            copy(hid_v.at[a, src], hid_v.at[a, src], h_ss.at[a, n], h_rs.at[a, n], (row, col)).wait_recv()
        hid = hid_v[a].reshape(block, units)
        for k, w in enumerate((wd_v, wdp_v)):
            mix = dot(hid, w[...])
            mix_f[a, k] = mix.reshape(4, share, width)
            mix_s[a, k] = mix.astype(BF16).reshape(4, share, width)
        ms.append([])
        for n, d in enumerate((2, 1, 3)):
            ms[a].append(
                copy(mix_s.at[a, :, (x + d) % 4], mix_r.at[a, n], m_ss.at[a, n], m_rs.at[a, n], (row, in_col(0, d)))
            )
            ms[a][-1].start()
    es = []
    for a in range(2):
        to = 2 * core + a
        here = z_hi == to
        mix = mix_f[a, :, x]
        for n in range(3):
            ms[a][n].wait_recv()
            mix = mix + mix_r[a, n].astype(F32)
        end_s[a] = mix.astype(BF16)
        cross = copy(end_s.at[a, 1], end_r.at[z_hi], e_ss.at[a, 1], e_rs.at[z_hi], (mate[0], to * 4 + x))
        same = copy(end_s.at[a, 0], end_r.at[z_hi], e_ss.at[a, 0], e_rs.at[z_hi], (row, to * 4 + x))
        pl.when(jnp.logical_not(here))(same.start)
        cross.start()

        @pl.when(here)
        def _():
            end_r[z_hi] = end_s[a, 0]

        es.append((same, cross, here))

    mine = z_hi // 2 == core
    for s in range(4):
        arrived = copy(end_r.at[s], end_r.at[s], e_ss.at[0, 0], e_rs.at[s], (row, col))
        pl.when(jnp.logical_not(mine & (z_hi == s)))(arrived.wait_recv)
    total = end_r[0].astype(F32)
    for s in range(1, 4):
        total = total + end_r[s].astype(F32)
    out[...] = total.astype(BF16)

    for c in l1 + l2 + pair + bs + gs + us[0] + us[1] + hs[0] + hs[1] + ms[0] + ms[1]:
        c.wait_send()
    for same, cross, here in es:
        pl.when(jnp.logical_not(here))(same.wait_send)
        cross.wait_send()


def shards(tokens, task_emb, gen_in, gen_a, gen_b, w_gate, w_up, w_down, group_count, group_task):
    batch, draft, width = tokens.shape
    hyper, slab, ranks = gen_a.shape
    groups = group_count.shape[0]
    units = w_gate.shape[1]
    n_tok = batch * draft
    half = n_tok // 2
    share = half // 8
    part = share // 2
    vm = pltpu.VMEM
    dma = pltpu.SemaphoreType.DMA
    args = (
        tokens,
        task_emb,
        gen_in,
        gen_a.transpose(1, 2, 0).reshape(slab * ranks, hyper),
        gen_b.reshape(hyper, units),
        w_gate,
        w_up,
        w_down,
        group_count.reshape(1, groups),
        group_task.reshape(1, groups),
    )
    scratch = [vm(a.shape, a.dtype) for a in args]
    scratch += [
        vm((n_tok, width), BF16),
        vm((half, width), BF16),
        vm((width, units), BF16),
        vm((width, units), BF16),
        vm((units, width), BF16),
        vm((2, 8, part, units), BF16),
        vm((ranks, part, units), BF16),
        vm((2, 8, 2, ranks * part), F32),
        vm((15, 2, ranks * part), F32),
        vm((2, ranks * part), F32),
        vm((15, 2, ranks * part), F32),
        vm((2, 8, part, units), BF16),
        vm((2, 8, part, units), BF16),
        vm((7, 2, part, units), BF16),
        vm((2, 7, part, units), BF16),
        vm((2, 8, part, units), BF16),
        vm((2, 2, 4, share, width), F32),
        vm((2, 2, 4, share, width), BF16),
        vm((2, 3, 2, share, width), BF16),
        vm((2, 2, share, width), BF16),
        vm((4, share, width), BF16),
        pltpu.SemaphoreType.REGULAR,
    ]
    scratch += [
        dma(n)
        for n in (
            (10,), (4,), (4,), (15,), (15,), (15,), (15,), (15,), (16,),
            (7,), (7,), (2, 7), (2, 7), (2, 7), (2, 7), (2, 3), (2, 3), (2, 2), (4,),
        )
    ]
    any_spec = pl.BlockSpec(memory_space=pl.ANY)
    out = pl.pallas_call(
        kernel,
        out_shape=jax.ShapeDtypeStruct((share, width), BF16),
        in_specs=[any_spec] * len(args),
        out_specs=pl.BlockSpec(memory_space=pltpu.VMEM),
        scratch_shapes=scratch,
        compiler_params=pltpu.CompilerParams(
            collective_id=0, has_side_effects=True, vmem_limit_bytes=32 * 1024 * 1024
        ),
    )(*[pltpu.with_memory_space_constraint(a, pltpu.HBM) for a in args])
    return out.reshape(share // draft, draft, width)


def solution(mesh):
    placed = (
        P(None, None, "row"),
        P(),
        P(),
        P(None, ("row", "col"), None),
        P(None, "row", "col"),
        P("row", "col"),
        P("row", "col"),
        P("col", "row"),
        P(),
        P(),
    )
    return jax.shard_map(
        shards, mesh=mesh, in_specs=placed, out_specs=P("col", None, "row"), check_vma=False
    )
```

```python
import functools

import jax
import jax.numpy as jnp
from jax import lax
from jax.experimental import pallas as pl
from jax.experimental.pallas import tpu as pltpu
from jax.sharding import PartitionSpec as P

MESH = pl.DeviceIdType.MESH
F32 = jnp.float32
BF16 = jnp.bfloat16


def dot(a, b, dims=((1,), (0,))):
    return lax.dot_general(a, b, (dims, ((), ())), preferred_element_type=F32)


def kernel(
    tokens, task_emb, gen_in, gen_a, gen_b, w_gate, w_up, w_down, count, task,
    out,
    tok3_v, emb_v, gin_v, ga_v, gb_v, wg_v, wu_v, wd_v, cnt_v, tsk_v,
    tok_v, tokp_v, wgp_v, wup_v, wdp_v, b_v,
    low_s, low1_r, low2_s, low2_r,
    gate_s, up_f, up_s, gate_r, up_r, hid_v, mix_f, mix_s, mix_r, end_s, end_r,
    known, load_sem, pair_ss, pair_rs, l1_ss, l1_rs, l2_ss, l2_rs,
    g_ss, g_rs, u_ss, u_rs, h_ss, h_rs, m_ss, m_rs, e_ss, e_rs,
):
    row = lax.axis_index("row")
    col = lax.axis_index("col")
    z_lo, y, core = row // 8, row // 2 % 4, row % 2
    z_hi, x = col // 4, col % 4
    chip = row // 2
    groups = count.shape[1]
    ranks = low_s.shape[1]
    mate = (row + 1 - 2 * core, col)

    def in_row(dz, dy, dk, sign=1):
        return ((z_lo + dz) % 2 * 4 + (y + sign * dy + 4) % 4) * 2 + (core + dk) % 2

    def in_col(dz, dx):
        return (z_hi + dz) % 4 * 4 + (x + dx) % 4

    row_steps = [(dz, dy, dk) for dz in (1, 0) for dy in (2, 1, 3, 0) for dk in (1, 0)][:-1]
    col_steps = [(dz, dx) for dz in (2, 1, 3, 0) for dx in (2, 1, 3, 0)][:-1]
    chip_steps = [(dz, dy) for dz in (1, 0) for dy in (2, 1, 3, 0)][:-1]

    bar = pltpu.get_barrier_semaphore()
    for d in (2, 1, 3):
        pl.semaphore_signal(bar, inc=1, device_id=(row, in_col(d, 0)), device_id_type=MESH)
    for step in row_steps:
        pl.semaphore_signal(bar, inc=1, device_id=(in_row(*step), col), device_id_type=MESH)
    for d in (2, 1, 3):
        pl.semaphore_signal(bar, inc=1, device_id=(row, in_col(0, d)), device_id_type=MESH)

    loads = [
        pltpu.make_async_copy(src, dst, load_sem.at[n])
        for n, (src, dst) in enumerate(
            [
                (task, tsk_v), (task_emb, emb_v), (gen_in, gin_v), (count, cnt_v), (gen_a, ga_v),
                (tokens, tok3_v), (gen_b, gb_v), (w_gate, wg_v), (w_up, wu_v), (w_down, wd_v),
            ]
        )
    ]
    for c in loads:
        c.start()

    def copy(src, dst, ss, rs, dev):
        return pltpu.make_async_remote_copy(
            src_ref=src, dst_ref=dst, send_sem=ss, recv_sem=rs, device_id=dev, device_id_type=MESH
        )

    gi = lax.broadcasted_iota(jnp.int32, (groups, groups), 0)
    gj = lax.broadcasted_iota(jnp.int32, (groups, groups), 1)
    loads[0].wait()
    task_of = jnp.sum(jnp.where(gi == gj, tsk_v[...].astype(F32), 0.0), axis=1, keepdims=True)
    tasks = emb_v.shape[0]
    pick = lax.broadcasted_iota(jnp.int32, (groups, tasks), 1).astype(F32) == task_of
    loads[1].wait()
    chosen = dot(jnp.where(pick, 1.0, 0.0).astype(BF16), emb_v[...]).astype(BF16)
    loads[2].wait()
    hyper = jax.nn.silu(dot(chosen, gin_v[...])).astype(BF16)

    loads[3].wait()
    cnt = cnt_v[...].astype(F32)
    ends = jnp.sum(jnp.where(gj <= gi, cnt, 0.0), axis=1, keepdims=True)
    starts = ends - jnp.sum(jnp.where(gj == gi, cnt, 0.0), axis=1, keepdims=True)

    def member(first, width):
        m = lax.broadcasted_iota(jnp.int32, (groups, width), 1) + first
        token = m // 64 % 4 * 128 + m // 16 % 4 * 32 + m // 256 * 16 + m % 16
        request = (token // 2).astype(F32)
        return jnp.where((request >= starts) & (request < ends), 1.0, 0.0)

    loads[4].wait()
    fac_a = dot(ga_v[...], hyper, ((1,), (1,))).astype(BF16)
    half, width = tok_v.shape[1:]
    n_tok = 2 * half
    slab = fac_a.shape[0] // ranks
    a_of = dot(fac_a, member(0, n_tok).astype(BF16))
    which = lax.broadcasted_iota(jnp.int32, (slab * ranks, width), 0) // ranks + col * slab
    sel = jnp.where(lax.broadcasted_iota(jnp.int32, (slab * ranks, width), 1) == which, 1.0, 0.0)
    loads[5].wait()
    tok = tok3_v[...].reshape(16, 2, n_tok // 32, width)
    for k in range(2):
        tok_v[k] = tok[:, k].reshape(half, width)
    t_of = dot(sel.astype(BF16), tok_v[...].reshape(n_tok, width), ((1,), (1,)))
    low = jnp.sum((a_of * t_of).reshape(slab, ranks, n_tok), axis=0)
    for h in range(2):
        for q in range(2):
            low_s[h, :, q, :] = low[:, h * 256 + q * 128 : h * 256 + q * 128 + 128]

    pl.semaphore_wait(bar, 21)
    for d in (2, 1, 3):
        pl.semaphore_signal(known, inc=1, device_id=(row, in_col(d, 0)), device_id_type=MESH)

    l1 = []
    for n, (dz, dy, dk) in enumerate(row_steps):
        to = in_row(dz, dy, dk)
        l1.append(
            copy(low_s.at[to % 2, pl.ds(to // 2 * 2, 2)], low1_r.at[n], l1_ss.at[n], l1_rs.at[n], (to, col))
        )
        l1[-1].start()
    for n in (7, 8, 9):
        loads[n].wait()
    pair = [
        copy(tok_v.at[1 - core], tokp_v, pair_ss.at[0], pair_rs.at[0], mate),
        copy(wg_v, wgp_v, pair_ss.at[1], pair_rs.at[1], mate),
        copy(wu_v, wup_v, pair_ss.at[2], pair_rs.at[2], mate),
        copy(wd_v, wdp_v, pair_ss.at[3], pair_rs.at[3], mate),
        copy(b_v.at[core], b_v.at[core], pair_ss.at[4], pair_rs.at[4], mate),
    ]
    for n in range(4):
        pair[n].start()
    loads[6].wait()
    b_v[core] = dot(hyper, gb_v[...]).astype(BF16)
    pair[4].start()

    gate = dot(tok_v[core], wg_v[...])
    pair[0].wait_recv()
    pair[1].wait_recv()
    part = half // 32
    units = gate.shape[1]
    gate_s[...] = (gate + dot(tokp_v[...], wgp_v[...])).astype(BF16).reshape(4, 8, part, units)

    def peer(dz, dy, sign=1):
        return in_row(dz, dy, 0, sign) // 2

    gs = []
    for n, (dz, dy) in enumerate(chip_steps):
        i = peer(dz, dy)
        gs.append(copy(gate_s.at[:, i], gate_r.at[n], g_ss.at[n], g_rs.at[n], (i * 2 + core, col)))
    for n, (dz, dy) in enumerate(chip_steps):
        if dz == 0:
            gs[n].start()

    low = low_s[core, pl.ds(chip * 2, 2)]
    for n in range(15):
        l1[n].wait_recv()
        low = low + low1_r[n]
    low2_s[...] = low
    pl.semaphore_wait(known, 3)
    l2 = []
    for n, (dz, dx) in enumerate(col_steps):
        l2.append(copy(low2_s, low2_r.at[n], l2_ss.at[n], l2_rs.at[n], (row, in_col(dz, dx))))
        l2[-1].start()
    for n, (dz, dy) in enumerate(chip_steps):
        if dz == 1:
            gs[n].start()

    up = dot(tok_v[core], wu_v[...])
    pair[2].wait_recv()
    up_f[...] = up + dot(tokp_v[...], wup_v[...])
    pair[4].wait_recv()
    b_all = b_v[...].reshape(2 * groups, units)
    block = half // 2
    mem = [member(core * half + a * block, block) for a in range(2)]
    for n in range(15):
        l2[n].wait_recv()
        low = low + low2_r[n]
    low = low.astype(BF16).astype(F32)
    us = []
    for q in range(4):
        us.append([])
        for n, (dz, dy) in enumerate(chip_steps):
            i = peer(dz, dy)
            us[q].append(
                copy(up_s.at[q, i], up_r.at[q, n], u_ss.at[q, n], u_rs.at[q, n], (i * 2 + core, col))
            )
    for a in range(2):
        spread = jnp.concatenate([mem[a] * low[r, a : a + 1, :] for r in range(2)], axis=0).astype(BF16)
        up = up_f[a * block : a * block + block, :] + dot(spread, b_all, ((0,), (0,)))
        up_s[2 * a : 2 * a + 2] = up.astype(BF16).reshape(2, 8, part, units)
        for q in (0, 1) if a == 0 else (2,):
            for c in us[q]:
                c.start()

    for n in range(7):
        gs[n].wait_recv()
    hs, ms, es = [], [], []

    def hidden(q):
        gate = gate_s[q, chip].astype(F32)
        for n in range(7):
            gate = gate + gate_r[n, q].astype(F32)
        act = jax.nn.silu(gate)
        up = up_s[q, chip].astype(F32)
        for n in range(7):
            us[q][n].wait_recv()
            up = up + up_r[q, n].astype(F32)
        hid_v[q, chip] = (act * up).astype(BF16)
        hs.append([])
        for n, (dz, dy) in enumerate(chip_steps):
            hs[q].append(
                copy(
                    hid_v.at[q, chip], hid_v.at[q, chip], h_ss.at[q, n], h_rs.at[q, n],
                    (peer(dz, dy) * 2 + core, col),
                )
            )
            hs[q][-1].start()

    rows = half // 16

    def partial(q):
        for n, (dz, dy) in enumerate(chip_steps):
            src = peer(dz, dy, -1)
            copy(hid_v.at[q, src], hid_v.at[q, src], h_ss.at[q, n], h_rs.at[q, n], (row, col)).wait_recv()
        hid = hid_v[q].reshape(8 * part, units)
        for k, w in enumerate((wd_v, wdp_v)):
            mix = dot(hid, w[...]).reshape(4, rows, width)
            mix_f[q, k] = mix
            mix_s[q, k] = mix.astype(BF16)
        ms.append([])
        for n, d in enumerate((2, 1, 3)):
            ms[q].append(
                copy(mix_s.at[q, :, (x + d) % 4], mix_r.at[q, n], m_ss.at[q, n], m_rs.at[q, n], (row, in_col(0, d)))
            )
            ms[q][-1].start()

    def end(q):
        here = z_hi == q
        mix = mix_f[q, :, x]
        for n in range(3):
            ms[q][n].wait_recv()
            mix = mix + mix_r[q, n].astype(F32)
        end_s[q] = mix.astype(BF16)
        slot = end_r.at[core, z_hi]
        cross = copy(end_s.at[q, 1], slot, e_ss.at[q, 1], e_rs.at[core, z_hi], (mate[0], q * 4 + x))
        same = copy(end_s.at[q, 0], slot, e_ss.at[q, 0], e_rs.at[core, z_hi], (row, q * 4 + x))
        pl.when(jnp.logical_not(here))(same.start)
        cross.start()

        @pl.when(here)
        def _():
            end_r[core, z_hi] = end_s[q, 0]

        es.append((same, cross, here))

    hidden(0)
    for c in us[3]:
        c.start()
    hidden(1)
    hidden(2)
    pair[3].wait_recv()
    partial(0)
    hidden(3)
    partial(1)
    end(0)
    partial(2)
    end(1)
    partial(3)
    end(2)
    end(3)

    for k in range(2):
        for s in range(4):
            arrived = copy(end_r.at[k, s], end_r.at[k, s], e_ss.at[0, 0], e_rs.at[k, s], (row, col))
            pl.when(jnp.logical_not((core == k) & (z_hi == s)))(arrived.wait_recv)
        total = end_r[k, 0].astype(F32)
        for s in range(1, 4):
            total = total + end_r[k, s].astype(F32)
        out[k * rows : k * rows + rows, :] = total.astype(BF16)

    for c in l1 + l2 + pair + gs + sum(us, []) + sum(hs, []) + sum(ms, []):
        c.wait_send()
    for same, cross, here in es:
        pl.when(jnp.logical_not(here))(same.wait_send)
        cross.wait_send()


def shards(tokens, task_emb, gen_in, gen_a, gen_b, w_gate, w_up, w_down, group_count, group_task):
    batch, draft, width = tokens.shape
    hyper, slab, ranks = gen_a.shape
    groups = group_count.shape[0]
    units = w_gate.shape[1]
    n_tok = batch * draft
    half = n_tok // 2
    share = half // 8
    part = half // 32
    rows = half // 16
    vm = pltpu.VMEM
    dma = pltpu.SemaphoreType.DMA
    args = (
        tokens,
        task_emb,
        gen_in,
        gen_a.transpose(1, 2, 0).reshape(slab * ranks, hyper),
        gen_b.reshape(hyper, units),
        w_gate,
        w_up,
        w_down,
        group_count.reshape(1, groups),
        group_task.reshape(1, groups),
    )
    scratch = [vm(a.shape, a.dtype) for a in args]
    scratch += [
        vm((2, half, width), BF16),
        vm((half, width), BF16),
        vm((width, units), BF16),
        vm((width, units), BF16),
        vm((units, width), BF16),
        vm((2, groups, units), BF16),
        vm((2, ranks, 2, half // 2), F32),
        vm((15, 2, 2, half // 2), F32),
        vm((2, 2, half // 2), F32),
        vm((15, 2, 2, half // 2), F32),
        vm((4, 8, part, units), BF16),
        vm((half, units), F32),
        vm((4, 8, part, units), BF16),
        vm((7, 4, part, units), BF16),
        vm((4, 7, part, units), BF16),
        vm((4, 8, part, units), BF16),
        vm((4, 2, 4, rows, width), F32),
        vm((4, 2, 4, rows, width), BF16),
        vm((4, 3, 2, rows, width), BF16),
        vm((4, 2, rows, width), BF16),
        vm((2, 4, rows, width), BF16),
        pltpu.SemaphoreType.REGULAR,
    ]
    scratch += [
        dma(n)
        for n in (
            (10,), (5,), (5,), (15,), (15,), (15,), (15,),
            (7,), (7,), (4, 7), (4, 7), (4, 7), (4, 7), (4, 3), (4, 3), (4, 2), (2, 4),
        )
    ]
    any_spec = pl.BlockSpec(memory_space=pl.ANY)
    out = pl.pallas_call(
        kernel,
        out_shape=jax.ShapeDtypeStruct((share, width), BF16),
        in_specs=[any_spec] * len(args),
        out_specs=pl.BlockSpec(memory_space=pltpu.VMEM),
        scratch_shapes=scratch,
        compiler_params=pltpu.CompilerParams(
            collective_id=0, has_side_effects=True, vmem_limit_bytes=32 * 1024 * 1024
        ),
    )(*[pltpu.with_memory_space_constraint(a, pltpu.HBM) for a in args])
    return out.reshape(share // draft, draft, width)


def solution(mesh):
    placed = (
        P(None, None, "row"),
        P(),
        P(),
        P(None, ("row", "col"), None),
        P(None, "row", "col"),
        P("row", "col"),
        P("row", "col"),
        P("col", "row"),
        P(),
        P(),
    )
    return jax.shard_map(
        shards, mesh=mesh, in_specs=placed, out_specs=P("col", None, "row"), check_vma=False
    )
```

```python
import functools

import jax
import jax.numpy as jnp
from jax import lax
from jax.experimental import pallas as pl
from jax.experimental.pallas import tpu as pltpu
from jax.sharding import PartitionSpec as P

MESH = pl.DeviceIdType.MESH
F32 = jnp.float32
BF16 = jnp.bfloat16


def dot(a, b, dims=((1,), (0,))):
    return lax.dot_general(a, b, (dims, ((), ())), preferred_element_type=F32)


def kernel(
    tokens, task_emb, gen_in, gen_a, gen_b, w_gate, w_up, w_down, count, task,
    out,
    tok3_v, emb_v, gin_v, ga_v, gb_v, wg_v, wu_v, wd_v, cnt_v, tsk_v,
    tok_v, tokp_v, wgp_v, wup_v, wdp_v, b_v,
    low_s, low1_r, low2_s, low2_r,
    gate_s, up_f, up_s, gate_r, up_r, hid_v, mix_f, mix_s, mix_r, end_s, end_r,
    known, load_sem, pair_ss, pair_rs, l1_ss, l1_rs, l2_ss, l2_rs,
    g_ss, g_rs, u_ss, u_rs, h_ss, h_rs, m_ss, m_rs, e_ss, e_rs,
):
    row = lax.axis_index("row")
    col = lax.axis_index("col")
    z_lo, y, core = row // 8, row // 2 % 4, row % 2
    z_hi, x = col // 4, col % 4
    chip = row // 2
    groups = count.shape[1]
    ranks = low_s.shape[1]
    mate = (row + 1 - 2 * core, col)

    def in_row(dz, dy, dk, sign=1):
        return ((z_lo + dz) % 2 * 4 + (y + sign * dy + 4) % 4) * 2 + (core + dk) % 2

    def in_col(dz, dx):
        return (z_hi + dz) % 4 * 4 + (x + dx) % 4

    row_steps = [(dz, dy, dk) for dz in (1, 0) for dy in (2, 1, 3, 0) for dk in (1, 0)][:-1]
    col_steps = [(dz, dx) for dz in (2, 1, 3, 0) for dx in (2, 1, 3, 0)][:-1]
    chip_steps = [(dz, dy) for dz in (1, 0) for dy in (2, 1, 3, 0)][:-1]

    bar = pltpu.get_barrier_semaphore()
    for d in (2, 1, 3):
        pl.semaphore_signal(bar, inc=1, device_id=(row, in_col(d, 0)), device_id_type=MESH)
    for step in row_steps:
        pl.semaphore_signal(bar, inc=1, device_id=(in_row(*step), col), device_id_type=MESH)
    for d in (2, 1, 3):
        pl.semaphore_signal(bar, inc=1, device_id=(row, in_col(0, d)), device_id_type=MESH)

    loads = [
        pltpu.make_async_copy(src, dst, load_sem.at[n])
        for n, (src, dst) in enumerate(
            [
                (task, tsk_v), (task_emb, emb_v), (gen_in, gin_v), (count, cnt_v), (gen_a, ga_v),
                (tokens, tok3_v), (gen_b, gb_v), (w_gate, wg_v), (w_up, wu_v), (w_down, wd_v),
            ]
        )
    ]
    for c in loads:
        c.start()

    def copy(src, dst, ss, rs, dev):
        return pltpu.make_async_remote_copy(
            src_ref=src, dst_ref=dst, send_sem=ss, recv_sem=rs, device_id=dev, device_id_type=MESH
        )

    def all_of(ref, ss, rs):
        return copy(ref, ref, ss, rs, (row, col))

    gi = lax.broadcasted_iota(jnp.int32, (groups, groups), 0)
    gj = lax.broadcasted_iota(jnp.int32, (groups, groups), 1)
    loads[0].wait()
    task_of = jnp.sum(jnp.where(gi == gj, tsk_v[...].astype(F32), 0.0), axis=1, keepdims=True)
    tasks = emb_v.shape[0]
    pick = lax.broadcasted_iota(jnp.int32, (groups, tasks), 1).astype(F32) == task_of
    loads[1].wait()
    chosen = dot(jnp.where(pick, 1.0, 0.0).astype(BF16), emb_v[...]).astype(BF16)
    loads[2].wait()
    hyper = jax.nn.silu(dot(chosen, gin_v[...])).astype(BF16)

    loads[3].wait()
    cnt = cnt_v[...].astype(F32)
    ends = jnp.sum(jnp.where(gj <= gi, cnt, 0.0), axis=1, keepdims=True)
    starts = ends - jnp.sum(jnp.where(gj == gi, cnt, 0.0), axis=1, keepdims=True)

    def member(first, width):
        m = lax.broadcasted_iota(jnp.int32, (groups, width), 1) + first
        request = ((m >> 6 & 3) << 6) + ((m >> 4 & 3) << 4) + ((m >> 8) << 3) + ((m & 15) >> 1)
        request = request.astype(F32)
        return jnp.where((request >= starts) & (request < ends), 1.0, 0.0)

    loads[4].wait()
    fac_a = dot(ga_v[...], hyper, ((1,), (1,))).astype(BF16)
    half, width = tokp_v.shape[0] * tokp_v.shape[1], tokp_v.shape[2]
    n_tok = 2 * half
    slab = fac_a.shape[0] // ranks
    a_of = dot(fac_a, member(0, n_tok).astype(BF16))
    which = (lax.broadcasted_iota(jnp.int32, (slab * ranks, width), 0) >> 4) + col * slab
    sel = jnp.where(lax.broadcasted_iota(jnp.int32, (slab * ranks, width), 1) == which, 1.0, 0.0)
    loads[5].wait()
    tok_v[...] = tok3_v[...].reshape(tok_v.shape)
    sel = sel.astype(BF16)
    for h in range(2):
        t_of = dot(sel, tok_v[:, h].reshape(half, width), ((1,), (1,)))
        low = jnp.sum((a_of[:, h * half : h * half + half] * t_of).reshape(slab, ranks, half), axis=0)
        for q in range(2):
            low_s[h, :, q, :] = low[:, q * 128 : q * 128 + 128]

    pl.semaphore_wait(bar, 21)
    for d in (2, 1, 3):
        pl.semaphore_signal(known, inc=1, device_id=(row, in_col(d, 0)), device_id_type=MESH)

    l1 = []
    for n, (dz, dy, dk) in enumerate(row_steps):
        to = in_row(dz, dy, dk)
        l1.append(
            copy(low_s.at[to % 2, pl.ds(to // 2 * 2, 2)], low1_r.at[n], l1_ss, l1_rs, (to, col))
        )
        l1[-1].start()
    for n in (7, 8, 9):
        loads[n].wait()
    pair = [
        copy(tok_v.at[:, 1 - core], tokp_v, pair_ss.at[0], pair_rs.at[0], mate),
        copy(wg_v, wgp_v, pair_ss.at[1], pair_rs.at[1], mate),
        copy(wu_v, wup_v, pair_ss.at[2], pair_rs.at[2], mate),
        copy(wd_v, wdp_v, pair_ss.at[3], pair_rs.at[3], mate),
        copy(b_v.at[core], b_v.at[core], pair_ss.at[4], pair_rs.at[4], mate),
    ]
    for n in range(4):
        pair[n].start()
    loads[6].wait()
    b_v[core] = dot(hyper, gb_v[...]).astype(BF16)
    pair[4].start()

    tok = tok_v[:, core].reshape(half, width)
    gate = dot(tok, wg_v[...])
    pair[0].wait_recv()
    pair[1].wait_recv()
    part = half // 32
    units = gate.shape[1]
    gate_s[...] = (gate + dot(tokp_v[...].reshape(half, width), wgp_v[...])).astype(BF16).reshape(4, 8, part, units)

    def peer(dz, dy, sign=1):
        return in_row(dz, dy, 0, sign) // 2

    gs = []
    for n, (dz, dy) in enumerate(chip_steps):
        i = peer(dz, dy)
        gs.append(copy(gate_s.at[:, i], gate_r.at[n], g_ss, g_rs, (i * 2 + core, col)))
    for n, (dz, dy) in enumerate(chip_steps):
        if dz == 0:
            gs[n].start()

    low = low_s[core, pl.ds(chip * 2, 2)]
    all_of(low1_r, l1_ss, l1_rs).wait_recv()
    low = low + jnp.sum(low1_r[...], axis=0)
    low2_s[...] = low
    pl.semaphore_wait(known, 3)
    l2 = []
    for n, (dz, dx) in enumerate(col_steps):
        l2.append(copy(low2_s, low2_r.at[n], l2_ss, l2_rs, (row, in_col(dz, dx))))
        l2[-1].start()
    for n, (dz, dy) in enumerate(chip_steps):
        if dz == 1:
            gs[n].start()

    up = dot(tok, wu_v[...])
    pair[2].wait_recv()
    up_f[...] = up + dot(tokp_v[...].reshape(half, width), wup_v[...])
    pair[4].wait_recv()
    b_all = b_v[...].reshape(2 * groups, units)
    block = half // 2
    mem = [member(core * half + a * block, block) for a in range(2)]
    all_of(low2_r, l2_ss, l2_rs).wait_recv()
    low = low + jnp.sum(low2_r[...], axis=0)
    low = low.astype(BF16).astype(F32)
    us = []
    for q in range(4):
        us.append([])
        for n, (dz, dy) in enumerate(chip_steps):
            i = peer(dz, dy)
            us[q].append(
                copy(up_s.at[q, i], up_r.at[q, n], u_ss.at[q], u_rs.at[q], (i * 2 + core, col))
            )
    for a in range(2):
        spread = jnp.concatenate([mem[a] * low[r, a : a + 1, :] for r in range(2)], axis=0).astype(BF16)
        up = up_f[a * block : a * block + block, :] + dot(spread, b_all, ((0,), (0,)))
        up_s[2 * a : 2 * a + 2] = up.astype(BF16).reshape(2, 8, part, units)
        for q in (0, 1) if a == 0 else (2,):
            for c in us[q]:
                c.start()

    all_of(gate_r, g_ss, g_rs).wait_recv()
    hs, ms = [], []

    def hidden(q):
        act = jax.nn.silu(gate_s[q, chip].astype(F32) + jnp.sum(gate_r[:, q].astype(F32), axis=0))
        all_of(up_r.at[q], u_ss.at[q], u_rs.at[q]).wait_recv()
        up = up_s[q, chip].astype(F32) + jnp.sum(up_r[q].astype(F32), axis=0)
        hid_v[q, chip] = (act * up).astype(BF16)
        hs.append([])
        for n, (dz, dy) in enumerate(chip_steps):
            hs[q].append(
                copy(
                    hid_v.at[q, chip], hid_v.at[q, chip], h_ss.at[q], h_rs.at[q],
                    (peer(dz, dy) * 2 + core, col),
                )
            )
            hs[q][-1].start()

    rows = half // 16

    def partial(q):
        all_of(hid_v.at[q, pl.ds(0, 7)], h_ss.at[q], h_rs.at[q]).wait_recv()
        hid = hid_v[q].reshape(8 * part, units)
        for k, w in enumerate((wd_v, wdp_v)):
            mix = dot(hid, w[...]).reshape(4, rows, width)
            mix_f[q, k] = mix
            mix_s[q, k] = mix.astype(BF16)
        ms.append([])
        for n, d in enumerate((2, 1, 3)):
            ms[q].append(
                copy(mix_s.at[q, :, (x + d) % 4], mix_r.at[q, n], m_ss.at[q], m_rs.at[q], (row, in_col(0, d)))
            )
            ms[q][-1].start()

    def end(q):
        here = z_hi == q
        all_of(mix_r.at[q], m_ss.at[q], m_rs.at[q]).wait_recv()
        end_s[q] = (mix_f[q, :, x] + jnp.sum(mix_r[q].astype(F32), axis=0)).astype(BF16)
        slot = end_r.at[core, z_hi]
        cross = copy(end_s.at[q, 1], slot, e_ss.at[1], e_rs.at[core], (mate[0], q * 4 + x))
        same = copy(end_s.at[q, 0], slot, e_ss.at[0], e_rs.at[core], (row, q * 4 + x))
        pl.when(jnp.logical_not(here))(same.start)
        cross.start()

        @pl.when(here)
        def _():
            end_r[core, z_hi] = end_s[q, 0]

    hidden(0)
    for c in us[3]:
        c.start()
    hidden(1)
    hidden(2)
    pair[3].wait_recv()
    partial(0)
    hidden(3)
    partial(1)
    end(0)
    partial(2)
    end(1)
    partial(3)
    end(2)
    end(3)

    for k in range(2):
        pl.when(core == k)(all_of(end_r.at[k, pl.ds(0, 3)], e_ss.at[0], e_rs.at[k]).wait_recv)
        pl.when(core != k)(all_of(end_r.at[k], e_ss.at[0], e_rs.at[k]).wait_recv)
        total = jnp.sum(end_r[k].astype(F32), axis=0)
        out[k * rows : k * rows + rows, :] = total.astype(BF16)

    for c in pair:
        c.wait_send()
    all_of(low1_r, l1_ss, l1_rs).wait_send()
    all_of(low2_r, l2_ss, l2_rs).wait_send()
    all_of(gate_r, g_ss, g_rs).wait_send()
    for q in range(4):
        all_of(up_r.at[q], u_ss.at[q], u_rs.at[q]).wait_send()
        all_of(hid_v.at[q, pl.ds(0, 7)], h_ss.at[q], h_rs.at[q]).wait_send()
        all_of(mix_r.at[q], m_ss.at[q], m_rs.at[q]).wait_send()
    all_of(end_s.at[pl.ds(0, 3), 0], e_ss.at[0], e_rs.at[0]).wait_send()
    all_of(end_s.at[:, 1], e_ss.at[1], e_rs.at[0]).wait_send()


def shards(tokens, task_emb, gen_in, gen_a, gen_b, w_gate, w_up, w_down, group_count, group_task):
    batch, draft, width = tokens.shape
    hyper, slab, ranks = gen_a.shape
    groups = group_count.shape[0]
    units = w_gate.shape[1]
    n_tok = batch * draft
    half = n_tok // 2
    share = half // 8
    part = half // 32
    rows = half // 16
    vm = pltpu.VMEM
    dma = pltpu.SemaphoreType.DMA
    args = (
        tokens,
        task_emb,
        gen_in,
        gen_a.transpose(1, 2, 0).reshape(slab * ranks, hyper),
        gen_b.reshape(hyper, units),
        w_gate,
        w_up,
        w_down,
        group_count.reshape(1, groups),
        group_task.reshape(1, groups),
    )
    scratch = [vm(a.shape, a.dtype) for a in args]
    scratch += [
        vm((16, 2, rows, width), BF16),
        vm((16, rows, width), BF16),
        vm((width, units), BF16),
        vm((width, units), BF16),
        vm((units, width), BF16),
        vm((2, groups, units), BF16),
        vm((2, ranks, 2, half // 2), F32),
        vm((15, 2, 2, half // 2), F32),
        vm((2, 2, half // 2), F32),
        vm((15, 2, 2, half // 2), F32),
        vm((4, 8, part, units), BF16),
        vm((half, units), F32),
        vm((4, 8, part, units), BF16),
        vm((7, 4, part, units), BF16),
        vm((4, 7, part, units), BF16),
        vm((4, 8, part, units), BF16),
        vm((4, 2, 4, rows, width), F32),
        vm((4, 2, 4, rows, width), BF16),
        vm((4, 3, 2, rows, width), BF16),
        vm((4, 2, rows, width), BF16),
        vm((2, 4, rows, width), BF16),
        pltpu.SemaphoreType.REGULAR,
    ]
    scratch += [dma((10,)), dma((5,)), dma((5,))] + [dma] * 6 + [dma((4,))] * 6 + [dma((2,))] * 2
    any_spec = pl.BlockSpec(memory_space=pl.ANY)
    out = pl.pallas_call(
        kernel,
        out_shape=jax.ShapeDtypeStruct((share, width), BF16),
        in_specs=[any_spec] * len(args),
        out_specs=pl.BlockSpec(memory_space=pltpu.VMEM),
        scratch_shapes=scratch,
        compiler_params=pltpu.CompilerParams(
            collective_id=0, has_side_effects=True, vmem_limit_bytes=32 * 1024 * 1024
        ),
    )(*[pltpu.with_memory_space_constraint(a, pltpu.HBM) for a in args])
    return out.reshape(share // draft, draft, width)


def solution(mesh):
    placed = (
        P(None, None, "row"),
        P(),
        P(),
        P(None, ("row", "col"), None),
        P(None, "row", "col"),
        P("row", "col"),
        P("row", "col"),
        P("col", "row"),
        P(),
        P(),
    )
    return jax.shard_map(
        shards, mesh=mesh, in_specs=placed, out_specs=P("col", None, "row"), check_vma=False
    )
```

```python
import functools

import jax
import jax.numpy as jnp
from jax import lax
from jax.experimental import pallas as pl
from jax.experimental.pallas import tpu as pltpu
from jax.sharding import PartitionSpec as P

MESH = pl.DeviceIdType.MESH
F32 = jnp.float32
BF16 = jnp.bfloat16


def dot(a, b, dims=((1,), (0,))):
    return lax.dot_general(a, b, (dims, ((), ())), preferred_element_type=F32)


def kernel(
    tokens, task_emb, gen_in, gen_a, gen_b, w_gate, w_up, w_down, count, task,
    out,
    tok3_v, emb_v, gin_v, ga_v, gb_v, wg_v, wu_v, wd_v, cnt_v, tsk_v,
    tok_v, tokp_v, wgp_v, wup_v, wdp_v, b_v,
    low_s, low1_r, low2_s, low2_r,
    gate_s, up_f, up_s, gate_r, up_r, hid_v, mix_f, mix_s, mix_r, end_s, end_r,
    known, load_sem, pair_ss, pair_rs, l1_ss, l1_rs, l2_ss, l2_rs,
    g_ss, g_rs, u_ss, u_rs, h_ss, h_rs, m_ss, m_rs, e_ss, e_rs,
):
    row = lax.axis_index("row")
    col = lax.axis_index("col")
    z_lo, y, core = row // 8, row // 2 % 4, row % 2
    z_hi, x = col // 4, col % 4
    chip = row // 2
    groups = count.shape[1]
    ranks = low_s.shape[1]
    mate = (row + 1 - 2 * core, col)

    def in_row(dz, dy, dk, sign=1):
        return ((z_lo + dz) % 2 * 4 + (y + sign * dy + 4) % 4) * 2 + (core + dk) % 2

    def in_col(dz, dx):
        return (z_hi + dz) % 4 * 4 + (x + dx) % 4

    row_steps = [(dz, dy, dk) for dz in (1, 0) for dy in (2, 1, 3, 0) for dk in (1, 0)][:-1]
    col_steps = [(dz, dx) for dz in (2, 1, 3, 0) for dx in (2, 1, 3, 0)][:-1]
    chip_steps = [(dz, dy) for dz in (1, 0) for dy in (2, 1, 3, 0)][:-1]

    bar = pltpu.get_barrier_semaphore()
    for d in (2, 1, 3):
        pl.semaphore_signal(bar, inc=1, device_id=(row, in_col(d, 0)), device_id_type=MESH)
    for step in row_steps:
        pl.semaphore_signal(bar, inc=1, device_id=(in_row(*step), col), device_id_type=MESH)
    for d in (2, 1, 3):
        pl.semaphore_signal(bar, inc=1, device_id=(row, in_col(0, d)), device_id_type=MESH)

    loads = [
        pltpu.make_async_copy(src, dst, load_sem.at[n])
        for n, (src, dst) in enumerate(
            [
                (task, tsk_v), (task_emb, emb_v), (gen_in, gin_v), (count, cnt_v), (gen_a, ga_v),
                (tokens, tok3_v), (gen_b, gb_v), (w_gate, wg_v), (w_up, wu_v), (w_down, wd_v),
            ]
        )
    ]
    for c in loads:
        c.start()

    def copy(src, dst, ss, rs, dev):
        return pltpu.make_async_remote_copy(
            src_ref=src, dst_ref=dst, send_sem=ss, recv_sem=rs, device_id=dev, device_id_type=MESH
        )

    def all_of(ref, ss, rs):
        return copy(ref, ref, ss, rs, (row, col))

    gi = lax.broadcasted_iota(jnp.int32, (groups, groups), 0)
    gj = lax.broadcasted_iota(jnp.int32, (groups, groups), 1)
    loads[0].wait()
    task_of = jnp.sum(jnp.where(gi == gj, tsk_v[...].astype(F32), 0.0), axis=1, keepdims=True)
    tasks = emb_v.shape[0]
    pick = lax.broadcasted_iota(jnp.int32, (groups, tasks), 1).astype(F32) == task_of
    loads[1].wait()
    chosen = dot(jnp.where(pick, 1.0, 0.0).astype(BF16), emb_v[...]).astype(BF16)
    loads[2].wait()
    hyper = jax.nn.silu(dot(chosen, gin_v[...])).astype(BF16)

    loads[3].wait()
    cnt = cnt_v[...].astype(F32)
    ends = jnp.sum(jnp.where(gj <= gi, cnt, 0.0), axis=1, keepdims=True)
    starts = ends - jnp.sum(jnp.where(gj == gi, cnt, 0.0), axis=1, keepdims=True)

    def member(first, width):
        m = lax.broadcasted_iota(jnp.int32, (groups, width), 1) + first
        request = ((m >> 6 & 3) << 6) + ((m >> 4 & 3) << 4) + ((m >> 8) << 3) + ((m & 15) >> 1)
        request = request.astype(F32)
        return jnp.where((request >= starts) & (request < ends), 1.0, 0.0)

    loads[4].wait()
    fac_a = dot(ga_v[...], hyper, ((1,), (1,))).astype(BF16)
    half, width = tokp_v.shape[0] * tokp_v.shape[1], tokp_v.shape[2]
    n_tok = 2 * half
    slab = fac_a.shape[0] // ranks
    a_of = dot(fac_a, member(0, n_tok).astype(BF16))
    which = (lax.broadcasted_iota(jnp.int32, (slab * ranks, width), 0) >> 4) + col * slab
    sel = jnp.where(lax.broadcasted_iota(jnp.int32, (slab * ranks, width), 1) == which, 1.0, 0.0)
    loads[5].wait()
    tok_v[...] = tok3_v[...].reshape(tok_v.shape)
    sel = sel.astype(BF16)
    for h in range(2):
        t_of = dot(sel, tok_v[:, h].reshape(half, width), ((1,), (1,)))
        low = jnp.sum((a_of[:, h * half : h * half + half] * t_of).reshape(slab, ranks, half), axis=0)
        for q in range(2):
            low_s[h, :, q, :] = low[:, q * 128 : q * 128 + 128]

    pl.semaphore_wait(bar, 21)
    for d in (2, 1, 3):
        pl.semaphore_signal(known, inc=1, device_id=(row, in_col(d, 0)), device_id_type=MESH)

    l1 = []
    for n, (dz, dy, dk) in enumerate(row_steps):
        to = in_row(dz, dy, dk)
        l1.append(
            copy(low_s.at[to % 2, pl.ds(to // 2 * 2, 2)], low1_r.at[n], l1_ss, l1_rs, (to, col))
        )
        l1[-1].start()
    for n in (7, 8, 9):
        loads[n].wait()
    pair = [
        copy(tok_v.at[:, 1 - core], tokp_v, pair_ss.at[0], pair_rs.at[0], mate),
        copy(wg_v, wgp_v, pair_ss.at[1], pair_rs.at[1], mate),
        copy(wu_v, wup_v, pair_ss.at[2], pair_rs.at[2], mate),
        copy(wd_v, wdp_v, pair_ss.at[3], pair_rs.at[3], mate),
        copy(b_v.at[core], b_v.at[core], pair_ss.at[4], pair_rs.at[4], mate),
    ]
    for n in range(4):
        pair[n].start()
    loads[6].wait()
    b_v[core] = dot(hyper, gb_v[...]).astype(BF16)
    pair[4].start()

    tok = tok_v[:, core].reshape(half, width)
    gate = dot(tok, wg_v[...])
    pair[0].wait_recv()
    pair[1].wait_recv()
    part = half // 32
    units = gate.shape[1]
    gate_s[...] = (gate + dot(tokp_v[...].reshape(half, width), wgp_v[...])).astype(BF16).reshape(4, 8, part, units)

    def peer(dz, dy, sign=1):
        return in_row(dz, dy, 0, sign) // 2

    gs = []
    for n, (dz, dy) in enumerate(chip_steps):
        i = peer(dz, dy)
        gs.append(copy(gate_s.at[:, i], gate_r.at[n], g_ss, g_rs, (i * 2 + core, col)))
    for n, (dz, dy) in enumerate(chip_steps):
        if dz == 0:
            gs[n].start()

    low = low_s[core, pl.ds(chip * 2, 2)]
    all_of(low1_r, l1_ss, l1_rs).wait_recv()
    low = low + jnp.sum(low1_r[...], axis=0)
    low2_s[...] = low
    pl.semaphore_wait(known, 3)
    l2 = []
    for n, (dz, dx) in enumerate(col_steps):
        l2.append(copy(low2_s, low2_r.at[n], l2_ss, l2_rs, (row, in_col(dz, dx))))
        l2[-1].start()
    for n, (dz, dy) in enumerate(chip_steps):
        if dz == 1:
            gs[n].start()

    up = dot(tok, wu_v[...])
    pair[2].wait_recv()
    up_f[...] = up + dot(tokp_v[...].reshape(half, width), wup_v[...])
    pair[4].wait_recv()
    b_all = b_v[...].reshape(2 * groups, units)
    block = half // 2
    mem = [member(core * half + a * block, block) for a in range(2)]
    all_of(low2_r, l2_ss, l2_rs).wait_recv()
    low = low + jnp.sum(low2_r[...], axis=0)
    low = low.astype(BF16).astype(F32)
    us = []
    for q in range(4):
        us.append([])
        for n, (dz, dy) in enumerate(chip_steps):
            i = peer(dz, dy)
            us[q].append(
                copy(up_s.at[q, i], up_r.at[q, n], u_ss, u_rs.at[q], (i * 2 + core, col))
            )
    for a in range(2):
        spread = jnp.concatenate([mem[a] * low[r, a : a + 1, :] for r in range(2)], axis=0).astype(BF16)
        up = up_f[a * block : a * block + block, :] + dot(spread, b_all, ((0,), (0,)))
        up_s[2 * a : 2 * a + 2] = up.astype(BF16).reshape(2, 8, part, units)
        for q in (0, 1) if a == 0 else (2,):
            for c in us[q]:
                c.start()

    all_of(gate_r, g_ss, g_rs).wait_recv()
    hs, ms = [], []

    def hidden(q):
        act = jax.nn.silu(gate_s[q, chip].astype(F32) + jnp.sum(gate_r[:, q].astype(F32), axis=0))
        all_of(up_r.at[q], u_ss, u_rs.at[q]).wait_recv()
        up = up_s[q, chip].astype(F32) + jnp.sum(up_r[q].astype(F32), axis=0)
        hid_v[q, chip] = (act * up).astype(BF16)
        hs.append([])
        for n, (dz, dy) in enumerate(chip_steps):
            hs[q].append(
                copy(
                    hid_v.at[q, chip], hid_v.at[q, chip], h_ss, h_rs.at[q],
                    (peer(dz, dy) * 2 + core, col),
                )
            )
            hs[q][-1].start()

    rows = half // 16

    def partial(q):
        all_of(hid_v.at[q, pl.ds(0, 7)], h_ss, h_rs.at[q]).wait_recv()
        hid = hid_v[q].reshape(8 * part, units)
        for k, w in enumerate((wd_v, wdp_v)):
            mix = dot(hid, w[...]).reshape(4, rows, width)
            mix_f[q, k] = mix
            mix_s[q, k] = mix.astype(BF16)
        ms.append([])
        for n, d in enumerate((2, 1, 3)):
            ms[q].append(
                copy(mix_s.at[q, :, (x + d) % 4], mix_r.at[q, n], m_ss, m_rs.at[q], (row, in_col(0, d)))
            )
            ms[q][-1].start()

    def end(q):
        here = z_hi == q
        all_of(mix_r.at[q], m_ss, m_rs.at[q]).wait_recv()
        end_s[q] = (mix_f[q, :, x] + jnp.sum(mix_r[q].astype(F32), axis=0)).astype(BF16)
        slot = end_r.at[core, z_hi]
        cross = copy(end_s.at[q, 1], slot, e_ss.at[1], e_rs.at[core], (mate[0], q * 4 + x))
        same = copy(end_s.at[q, 0], slot, e_ss.at[0], e_rs.at[core], (row, q * 4 + x))
        pl.when(jnp.logical_not(here))(same.start)
        cross.start()

        @pl.when(here)
        def _():
            end_r[core, z_hi] = end_s[q, 0]

    hidden(0)
    for c in us[3]:
        c.start()
    hidden(1)
    hidden(2)
    pair[3].wait_recv()
    partial(0)
    hidden(3)
    partial(1)
    partial(2)
    end(0)
    partial(3)
    end(1)
    end(2)
    end(3)

    for k in range(2):
        pl.when(core == k)(all_of(end_r.at[k, pl.ds(0, 3)], e_ss.at[0], e_rs.at[k]).wait_recv)
        pl.when(core != k)(all_of(end_r.at[k], e_ss.at[0], e_rs.at[k]).wait_recv)
        total = jnp.sum(end_r[k].astype(F32), axis=0)
        out[k * rows : k * rows + rows, :] = total.astype(BF16)

    for c in pair:
        c.wait_send()
    all_of(low1_r, l1_ss, l1_rs).wait_send()
    all_of(low2_r, l2_ss, l2_rs).wait_send()
    all_of(gate_r, g_ss, g_rs).wait_send()
    all_of(up_r, u_ss, u_rs.at[0]).wait_send()
    all_of(hid_v.at[:, pl.ds(0, 7)], h_ss, h_rs.at[0]).wait_send()
    all_of(mix_r, m_ss, m_rs.at[0]).wait_send()
    all_of(end_s.at[pl.ds(0, 3), 0], e_ss.at[0], e_rs.at[0]).wait_send()
    all_of(end_s.at[:, 1], e_ss.at[1], e_rs.at[0]).wait_send()


def shards(tokens, task_emb, gen_in, gen_a, gen_b, w_gate, w_up, w_down, group_count, group_task):
    batch, draft, width = tokens.shape
    hyper, slab, ranks = gen_a.shape
    groups = group_count.shape[0]
    units = w_gate.shape[1]
    n_tok = batch * draft
    half = n_tok // 2
    share = half // 8
    part = half // 32
    rows = half // 16
    vm = pltpu.VMEM
    dma = pltpu.SemaphoreType.DMA
    args = (
        tokens,
        task_emb,
        gen_in,
        gen_a.transpose(1, 2, 0).reshape(slab * ranks, hyper),
        gen_b.reshape(hyper, units),
        w_gate,
        w_up,
        w_down,
        group_count.reshape(1, groups),
        group_task.reshape(1, groups),
    )
    scratch = [vm(a.shape, a.dtype) for a in args]
    scratch += [
        vm((16, 2, rows, width), BF16),
        vm((16, rows, width), BF16),
        vm((width, units), BF16),
        vm((width, units), BF16),
        vm((units, width), BF16),
        vm((2, groups, units), BF16),
        vm((2, ranks, 2, half // 2), F32),
        vm((15, 2, 2, half // 2), F32),
        vm((2, 2, half // 2), F32),
        vm((15, 2, 2, half // 2), F32),
        vm((4, 8, part, units), BF16),
        vm((half, units), F32),
        vm((4, 8, part, units), BF16),
        vm((7, 4, part, units), BF16),
        vm((4, 7, part, units), BF16),
        vm((4, 8, part, units), BF16),
        vm((4, 2, 4, rows, width), F32),
        vm((4, 2, 4, rows, width), BF16),
        vm((4, 3, 2, rows, width), BF16),
        vm((4, 2, rows, width), BF16),
        vm((2, 4, rows, width), BF16),
        pltpu.SemaphoreType.REGULAR,
    ]
    scratch += [dma((10,)), dma((5,)), dma((5,))] + [dma] * 6 + [dma, dma((4,))] * 3 + [dma((2,))] * 2
    any_spec = pl.BlockSpec(memory_space=pl.ANY)
    out = pl.pallas_call(
        kernel,
        out_shape=jax.ShapeDtypeStruct((share, width), BF16),
        in_specs=[any_spec] * len(args),
        out_specs=pl.BlockSpec(memory_space=pltpu.VMEM),
        scratch_shapes=scratch,
        compiler_params=pltpu.CompilerParams(
            collective_id=0, has_side_effects=True, vmem_limit_bytes=32 * 1024 * 1024
        ),
    )(*[pltpu.with_memory_space_constraint(a, pltpu.HBM) for a in args])
    return out.reshape(share // draft, draft, width)


def solution(mesh):
    placed = (
        P(None, None, "row"),
        P(),
        P(),
        P(None, ("row", "col"), None),
        P(None, "row", "col"),
        P("row", "col"),
        P("row", "col"),
        P("col", "row"),
        P(),
        P(),
    )
    return jax.shard_map(
        shards, mesh=mesh, in_specs=placed, out_specs=P("col", None, "row"), check_vma=False
    )
```

```python
import functools

import jax
import jax.numpy as jnp
from jax import lax
from jax.experimental import pallas as pl
from jax.experimental.pallas import tpu as pltpu
from jax.sharding import PartitionSpec as P

MESH = pl.DeviceIdType.MESH
F32 = jnp.float32
BF16 = jnp.bfloat16


def dot(a, b, dims=((1,), (0,))):
    return lax.dot_general(a, b, (dims, ((), ())), preferred_element_type=F32)


def kernel(
    tokens, task_emb, gen_in, gen_a, gen_b, w_gate, w_up, w_down, count, task,
    out,
    tok3_v, emb_v, gin_v, ga_v, gb_v, wg_v, wu_v, wd_v, cnt_v, tsk_v,
    tok_v, tokp_v, wgp_v, wup_v, wdp_v, b_v,
    low_s, low1_r, low2_s, low2_r,
    gate_s, up_f, up_s, gate_r, up_r, hid_v, mix_f, mix_s, mix_r, end_s, end_r,
    known, load_sem, pair_ss, pair_rs, l1_ss, l1_rs, l2_ss, l2_rs,
    g_ss, g_rs, u_ss, u_rs, h_ss, h_rs, m_ss, m_rs, e_ss, e_rs,
):
    row = lax.axis_index("row")
    col = lax.axis_index("col")
    z_lo, y, core = row // 8, row // 2 % 4, row % 2
    z_hi, x = col // 4, col % 4
    chip = row // 2
    groups = count.shape[1]
    ranks = low_s.shape[1]
    mate = (row + 1 - 2 * core, col)

    def in_row(dz, dy, dk, sign=1):
        return ((z_lo + dz) % 2 * 4 + (y + sign * dy + 4) % 4) * 2 + (core + dk) % 2

    def in_col(dz, dx):
        return (z_hi + dz) % 4 * 4 + (x + dx) % 4

    row_steps = [(dz, dy, dk) for dz in (1, 0) for dy in (2, 1, 3, 0) for dk in (1, 0)][:-1]
    col_steps = [(dz, dx) for dz in (2, 1, 3, 0) for dx in (2, 1, 3, 0)][:-1]
    chip_steps = [(1, 2), (0, 2), (1, 1), (0, 1), (1, 3), (0, 3), (1, 0)]

    bar = pltpu.get_barrier_semaphore()
    for d in (2, 1, 3):
        pl.semaphore_signal(bar, inc=1, device_id=(row, in_col(d, 0)), device_id_type=MESH)
    for step in row_steps:
        pl.semaphore_signal(bar, inc=1, device_id=(in_row(*step), col), device_id_type=MESH)
    for d in (2, 1, 3):
        pl.semaphore_signal(bar, inc=1, device_id=(row, in_col(0, d)), device_id_type=MESH)

    loads = [
        pltpu.make_async_copy(src, dst, load_sem.at[n])
        for n, (src, dst) in enumerate(
            [
                (task, tsk_v), (task_emb, emb_v), (gen_in, gin_v), (count, cnt_v), (gen_a, ga_v),
                (tokens, tok3_v), (gen_b, gb_v), (w_gate, wg_v), (w_up, wu_v), (w_down, wd_v),
            ]
        )
    ]
    for c in loads:
        c.start()

    def copy(src, dst, ss, rs, dev):
        return pltpu.make_async_remote_copy(
            src_ref=src, dst_ref=dst, send_sem=ss, recv_sem=rs, device_id=dev, device_id_type=MESH
        )

    def all_of(ref, ss, rs):
        return copy(ref, ref, ss, rs, (row, col))

    gi = lax.broadcasted_iota(jnp.int32, (groups, groups), 0)
    gj = lax.broadcasted_iota(jnp.int32, (groups, groups), 1)
    loads[0].wait()
    task_of = jnp.sum(jnp.where(gi == gj, tsk_v[...].astype(F32), 0.0), axis=1, keepdims=True)
    tasks = emb_v.shape[0]
    pick = lax.broadcasted_iota(jnp.int32, (groups, tasks), 1).astype(F32) == task_of
    loads[1].wait()
    chosen = dot(jnp.where(pick, 1.0, 0.0).astype(BF16), emb_v[...]).astype(BF16)
    loads[2].wait()
    hyper = jax.nn.silu(dot(chosen, gin_v[...])).astype(BF16)

    loads[3].wait()
    cnt = cnt_v[...].astype(F32)
    ends = jnp.sum(jnp.where(gj <= gi, cnt, 0.0), axis=1, keepdims=True)
    starts = ends - jnp.sum(jnp.where(gj == gi, cnt, 0.0), axis=1, keepdims=True)

    def member(first, width):
        m = lax.broadcasted_iota(jnp.int32, (groups, width), 1) + first
        request = ((m >> 6 & 3) << 6) + ((m >> 4 & 3) << 4) + ((m >> 8) << 3) + ((m & 15) >> 1)
        request = request.astype(F32)
        return jnp.where((request >= starts) & (request < ends), 1.0, 0.0)

    loads[4].wait()
    fac_a = dot(ga_v[...], hyper, ((1,), (1,))).astype(BF16)
    half, width = tokp_v.shape[0] * tokp_v.shape[1], tokp_v.shape[2]
    n_tok = 2 * half
    slab = fac_a.shape[0] // ranks
    a_of = dot(fac_a, member(0, n_tok).astype(BF16))
    which = (lax.broadcasted_iota(jnp.int32, (slab * ranks, width), 0) >> 4) + col * slab
    sel = jnp.where(lax.broadcasted_iota(jnp.int32, (slab * ranks, width), 1) == which, 1.0, 0.0)
    loads[5].wait()
    tok_v[...] = tok3_v[...].reshape(tok_v.shape)
    sel = sel.astype(BF16)
    for h in range(2):
        t_of = dot(sel, tok_v[:, h].reshape(half, width), ((1,), (1,)))
        low = jnp.sum((a_of[:, h * half : h * half + half] * t_of).reshape(slab, ranks, half), axis=0)
        for q in range(2):
            low_s[h, :, q, :] = low[:, q * 128 : q * 128 + 128]

    pl.semaphore_wait(bar, 21)
    for d in (2, 1, 3):
        pl.semaphore_signal(known, inc=1, device_id=(row, in_col(d, 0)), device_id_type=MESH)

    l1 = []
    for n, (dz, dy, dk) in enumerate(row_steps):
        to = in_row(dz, dy, dk)
        l1.append(
            copy(low_s.at[to % 2, pl.ds(to // 2 * 2, 2)], low1_r.at[n], l1_ss, l1_rs, (to, col))
        )
        l1[-1].start()
    for n in (7, 8, 9):
        loads[n].wait()
    pair = [
        copy(tok_v.at[:, 1 - core], tokp_v, pair_ss.at[0], pair_rs.at[0], mate),
        copy(wg_v, wgp_v, pair_ss.at[1], pair_rs.at[1], mate),
        copy(wu_v, wup_v, pair_ss.at[2], pair_rs.at[2], mate),
        copy(wd_v, wdp_v, pair_ss.at[3], pair_rs.at[3], mate),
        copy(b_v.at[core], b_v.at[core], pair_ss.at[4], pair_rs.at[4], mate),
    ]
    for n in range(2):
        pair[n].start()
    loads[6].wait()
    b_v[core] = dot(hyper, gb_v[...]).astype(BF16)
    pair[4].start()

    tok = tok_v[:, core].reshape(half, width)
    gate = dot(tok, wg_v[...])
    pair[0].wait_recv()
    pair[1].wait_recv()
    part = half // 32
    units = gate.shape[1]
    gate_s[...] = (gate + dot(tokp_v[...].reshape(half, width), wgp_v[...])).astype(BF16).reshape(4, 8, part, units)

    def peer(dz, dy, sign=1):
        return in_row(dz, dy, 0, sign) // 2

    gs = []
    for n, (dz, dy) in enumerate(chip_steps):
        i = peer(dz, dy)
        gs.append(copy(gate_s.at[:, i], gate_r.at[n], g_ss, g_rs, (i * 2 + core, col)))
    for n, (dz, dy) in enumerate(chip_steps):
        if dz == 0:
            gs[n].start()

    low = low_s[core, pl.ds(chip * 2, 2)]
    all_of(low1_r, l1_ss, l1_rs).wait_recv()
    low = low + jnp.sum(low1_r[...], axis=0)
    low2_s[...] = low
    pl.semaphore_wait(known, 3)
    l2 = []
    for n, (dz, dx) in enumerate(col_steps):
        l2.append(copy(low2_s, low2_r.at[n], l2_ss, l2_rs, (row, in_col(dz, dx))))
        l2[-1].start()
    for n, (dz, dy) in enumerate(chip_steps):
        if dz == 1:
            gs[n].start()
    pair[2].start()
    pair[3].start()

    up = dot(tok, wu_v[...])
    pair[2].wait_recv()
    up_f[...] = up + dot(tokp_v[...].reshape(half, width), wup_v[...])
    pair[4].wait_recv()
    b_all = b_v[...].reshape(2 * groups, units)
    block = half // 2
    mem = [member(core * half + a * block, block) for a in range(2)]
    all_of(low2_r, l2_ss, l2_rs).wait_recv()
    low = low + jnp.sum(low2_r[...], axis=0)
    low = low.astype(BF16).astype(F32)
    us = []
    for q in range(4):
        us.append([])
        for n, (dz, dy) in enumerate(chip_steps):
            i = peer(dz, dy)
            us[q].append(
                copy(up_s.at[q, i], up_r.at[q, n], u_ss, u_rs.at[q], (i * 2 + core, col))
            )
    for q in range(4):
        quarter = slice(q % 2 * 64, q % 2 * 64 + 64)
        spread = jnp.concatenate(
            [mem[q // 2][:, quarter] * low[r, q // 2 : q // 2 + 1, quarter] for r in range(2)], axis=0
        ).astype(BF16)
        up = up_f[q * 64 : q * 64 + 64, :] + dot(spread, b_all, ((0,), (0,)))
        up_s[q] = up.astype(BF16).reshape(8, part, units)
        if q < 3:
            for c in us[q]:
                c.start()

    all_of(gate_r, g_ss, g_rs).wait_recv()
    hs, ms = [], []

    def hidden(q):
        act = jax.nn.silu(gate_s[q, chip].astype(F32) + jnp.sum(gate_r[:, q].astype(F32), axis=0))
        all_of(up_r.at[q], u_ss, u_rs.at[q]).wait_recv()
        up = up_s[q, chip].astype(F32) + jnp.sum(up_r[q].astype(F32), axis=0)
        hid_v[q, chip] = (act * up).astype(BF16)
        hs.append([])
        for n, (dz, dy) in enumerate(chip_steps):
            hs[q].append(
                copy(
                    hid_v.at[q, chip], hid_v.at[q, chip], h_ss, h_rs.at[q],
                    (peer(dz, dy) * 2 + core, col),
                )
            )
            hs[q][-1].start()

    rows = half // 16

    def partial(q):
        all_of(hid_v.at[q, pl.ds(0, 7)], h_ss, h_rs.at[q]).wait_recv()
        hid = hid_v[q].reshape(8 * part, units)
        for k, w in enumerate((wd_v, wdp_v)):
            mix = dot(hid, w[...]).reshape(4, rows, width)
            mix_f[q, k] = mix
            mix_s[q, k] = mix.astype(BF16)
        ms.append([])
        for n, d in enumerate((2, 1, 3)):
            ms[q].append(
                copy(mix_s.at[q, :, (x + d) % 4], mix_r.at[q, n], m_ss, m_rs.at[q], (row, in_col(0, d)))
            )
            ms[q][-1].start()

    def end(q):
        here = z_hi == q
        all_of(mix_r.at[q], m_ss, m_rs.at[q]).wait_recv()
        end_s[q] = (mix_f[q, :, x] + jnp.sum(mix_r[q].astype(F32), axis=0)).astype(BF16)
        slot = end_r.at[core, z_hi]
        cross = copy(end_s.at[q, 1], slot, e_ss.at[1], e_rs.at[core], (mate[0], q * 4 + x))
        same = copy(end_s.at[q, 0], slot, e_ss.at[0], e_rs.at[core], (row, q * 4 + x))
        pl.when(jnp.logical_not(here))(same.start)
        cross.start()

        @pl.when(here)
        def _():
            end_r[core, z_hi] = end_s[q, 0]

    hidden(0)
    for c in us[3]:
        c.start()
    hidden(1)
    hidden(2)
    pair[3].wait_recv()
    partial(0)
    hidden(3)
    partial(1)
    partial(2)
    end(0)
    partial(3)
    end(1)
    end(2)
    end(3)

    for k in range(2):
        pl.when(core == k)(all_of(end_r.at[k, pl.ds(0, 3)], e_ss.at[0], e_rs.at[k]).wait_recv)
        pl.when(core != k)(all_of(end_r.at[k], e_ss.at[0], e_rs.at[k]).wait_recv)
        total = jnp.sum(end_r[k].astype(F32), axis=0)
        out[k * rows : k * rows + rows, :] = total.astype(BF16)

    for c in pair:
        c.wait_send()
    all_of(low1_r, l1_ss, l1_rs).wait_send()
    all_of(low2_r, l2_ss, l2_rs).wait_send()
    all_of(gate_r, g_ss, g_rs).wait_send()
    all_of(up_r, u_ss, u_rs.at[0]).wait_send()
    all_of(hid_v.at[:, pl.ds(0, 7)], h_ss, h_rs.at[0]).wait_send()
    all_of(mix_r, m_ss, m_rs.at[0]).wait_send()
    all_of(end_s.at[pl.ds(0, 3), 0], e_ss.at[0], e_rs.at[0]).wait_send()
    all_of(end_s.at[:, 1], e_ss.at[1], e_rs.at[0]).wait_send()


def shards(tokens, task_emb, gen_in, gen_a, gen_b, w_gate, w_up, w_down, group_count, group_task):
    batch, draft, width = tokens.shape
    hyper, slab, ranks = gen_a.shape
    groups = group_count.shape[0]
    units = w_gate.shape[1]
    n_tok = batch * draft
    half = n_tok // 2
    share = half // 8
    part = half // 32
    rows = half // 16
    vm = pltpu.VMEM
    dma = pltpu.SemaphoreType.DMA
    args = (
        tokens,
        task_emb,
        gen_in,
        gen_a.transpose(1, 2, 0).reshape(slab * ranks, hyper),
        gen_b.reshape(hyper, units),
        w_gate,
        w_up,
        w_down,
        group_count.reshape(1, groups),
        group_task.reshape(1, groups),
    )
    scratch = [vm(a.shape, a.dtype) for a in args]
    scratch += [
        vm((16, 2, rows, width), BF16),
        vm((16, rows, width), BF16),
        vm((width, units), BF16),
        vm((width, units), BF16),
        vm((units, width), BF16),
        vm((2, groups, units), BF16),
        vm((2, ranks, 2, half // 2), F32),
        vm((15, 2, 2, half // 2), F32),
        vm((2, 2, half // 2), F32),
        vm((15, 2, 2, half // 2), F32),
        vm((4, 8, part, units), BF16),
        vm((half, units), F32),
        vm((4, 8, part, units), BF16),
        vm((7, 4, part, units), BF16),
        vm((4, 7, part, units), BF16),
        vm((4, 8, part, units), BF16),
        vm((4, 2, 4, rows, width), F32),
        vm((4, 2, 4, rows, width), BF16),
        vm((4, 3, 2, rows, width), BF16),
        vm((4, 2, rows, width), BF16),
        vm((2, 4, rows, width), BF16),
        pltpu.SemaphoreType.REGULAR,
    ]
    scratch += [dma((10,)), dma((5,)), dma((5,))] + [dma] * 6 + [dma, dma((4,))] * 3 + [dma((2,))] * 2
    any_spec = pl.BlockSpec(memory_space=pl.ANY)
    out = pl.pallas_call(
        kernel,
        out_shape=jax.ShapeDtypeStruct((share, width), BF16),
        in_specs=[any_spec] * len(args),
        out_specs=pl.BlockSpec(memory_space=pltpu.VMEM),
        scratch_shapes=scratch,
        compiler_params=pltpu.CompilerParams(
            collective_id=0, has_side_effects=True, vmem_limit_bytes=32 * 1024 * 1024
        ),
    )(*[pltpu.with_memory_space_constraint(a, pltpu.HBM) for a in args])
    return out.reshape(share // draft, draft, width)


def solution(mesh):
    placed = (
        P(None, None, "row"),
        P(),
        P(),
        P(None, ("row", "col"), None),
        P(None, "row", "col"),
        P("row", "col"),
        P("row", "col"),
        P("col", "row"),
        P(),
        P(),
    )
    return jax.shard_map(
        shards, mesh=mesh, in_specs=placed, out_specs=P("col", None, "row"), check_vma=False
    )
```

```python
import functools

import jax
import jax.numpy as jnp
from jax import lax
from jax.experimental import pallas as pl
from jax.experimental.pallas import tpu as pltpu
from jax.sharding import PartitionSpec as P

MESH = pl.DeviceIdType.MESH
F32 = jnp.float32
BF16 = jnp.bfloat16


def dot(a, b, dims=((1,), (0,))):
    return lax.dot_general(a, b, (dims, ((), ())), preferred_element_type=F32)


def kernel(
    tokens, task_emb, gen_in, gen_a, gen_b, w_gate, w_up, w_down, count, task,
    out,
    tok3_v, emb_v, gin_v, ga_v, gb_v, wg_v, wu_v, wd_v, cnt_v, tsk_v,
    tok_v, tokp_v, wgp_v, wup_v, wdp_v, b_v,
    low_s, low1_r, low2_s, low2_r,
    gate_s, up_f, up_s, gate_r, up_r, hid_v, mix_f, mix_s, mix_r, end_s, end_r,
    known, load_sem, pair_ss, pair_rs, l1_ss, l1_rs, l2_ss, l2_rs,
    g_ss, g_rs, u_ss, u_rs, h_ss, h_rs, m_ss, m_rs, e_ss, e_rs,
):
    row = lax.axis_index("row")
    col = lax.axis_index("col")
    z_lo, y, core = row // 8, row // 2 % 4, row % 2
    z_hi, x = col // 4, col % 4
    chip = row // 2
    groups = count.shape[1]
    ranks = low_s.shape[1]
    mate = (row + 1 - 2 * core, col)

    def in_row(dz, dy, dk, sign=1):
        return ((z_lo + dz) % 2 * 4 + (y + sign * dy + 4) % 4) * 2 + (core + dk) % 2

    def in_col(dz, dx):
        return (z_hi + dz) % 4 * 4 + (x + dx) % 4

    row_steps = [(dz, dy, dk) for dz in (1, 0) for dy in (2, 1, 3, 0) for dk in (1, 0)][:-1]
    col_steps = [(dz, dx) for dz in (2, 1, 3, 0) for dx in (2, 1, 3, 0)][:-1]
    chip_steps = [(1, 2), (0, 2), (1, 1), (0, 1), (1, 3), (0, 3), (1, 0)]

    bar = pltpu.get_barrier_semaphore()
    for d in (2, 1, 3):
        pl.semaphore_signal(bar, inc=1, device_id=(row, in_col(d, 0)), device_id_type=MESH)
    for step in row_steps:
        pl.semaphore_signal(bar, inc=1, device_id=(in_row(*step), col), device_id_type=MESH)
    for d in (2, 1, 3):
        pl.semaphore_signal(bar, inc=1, device_id=(row, in_col(0, d)), device_id_type=MESH)

    loads = [
        pltpu.make_async_copy(src, dst, load_sem.at[n])
        for n, (src, dst) in enumerate(
            [
                (task, tsk_v), (task_emb, emb_v), (gen_in, gin_v), (count, cnt_v), (gen_a, ga_v),
                (tokens, tok3_v), (gen_b, gb_v), (w_gate, wg_v), (w_up, wu_v), (w_down, wd_v),
            ]
        )
    ]
    for c in loads:
        c.start()

    def copy(src, dst, ss, rs, dev):
        return pltpu.make_async_remote_copy(
            src_ref=src, dst_ref=dst, send_sem=ss, recv_sem=rs, device_id=dev, device_id_type=MESH
        )

    def all_of(ref, ss, rs):
        return copy(ref, ref, ss, rs, (row, col))

    gi = lax.broadcasted_iota(jnp.int32, (groups, groups), 0)
    gj = lax.broadcasted_iota(jnp.int32, (groups, groups), 1)
    loads[0].wait()
    task_of = jnp.sum(jnp.where(gi == gj, tsk_v[...].astype(F32), 0.0), axis=1, keepdims=True)
    tasks = emb_v.shape[0]
    pick = lax.broadcasted_iota(jnp.int32, (groups, tasks), 1).astype(F32) == task_of
    loads[1].wait()
    chosen = dot(jnp.where(pick, 1.0, 0.0).astype(BF16), emb_v[...]).astype(BF16)
    loads[2].wait()
    hyper = jax.nn.silu(dot(chosen, gin_v[...])).astype(BF16)

    loads[3].wait()
    cnt = cnt_v[...].astype(F32)
    ends = jnp.sum(jnp.where(gj <= gi, cnt, 0.0), axis=1, keepdims=True)
    starts = ends - jnp.sum(jnp.where(gj == gi, cnt, 0.0), axis=1, keepdims=True)

    def member(first, width):
        m = lax.broadcasted_iota(jnp.int32, (groups, width), 1) + first
        request = ((m >> 6 & 3) << 6) + ((m >> 4 & 3) << 4) + ((m >> 8) << 3) + ((m & 15) >> 1)
        request = request.astype(F32)
        return jnp.where((request >= starts) & (request < ends), 1.0, 0.0)

    loads[4].wait()
    fac_a = dot(ga_v[...], hyper, ((1,), (1,))).astype(BF16)
    half, width = tokp_v.shape[0] * tokp_v.shape[1], tokp_v.shape[2]
    n_tok = 2 * half
    slab = fac_a.shape[0] // ranks
    a_of = dot(fac_a, member(0, n_tok).astype(BF16))
    which = (lax.broadcasted_iota(jnp.int32, (slab * ranks, width), 0) >> 4) + col * slab
    sel = jnp.where(lax.broadcasted_iota(jnp.int32, (slab * ranks, width), 1) == which, 1.0, 0.0)
    loads[5].wait()
    tok_v[...] = tok3_v[...].reshape(tok_v.shape)
    sel = sel.astype(BF16)
    for h in range(2):
        t_of = dot(sel, tok_v[:, h].reshape(half, width), ((1,), (1,)))
        low = jnp.sum((a_of[:, h * half : h * half + half] * t_of).reshape(slab, ranks, half), axis=0)
        for q in range(2):
            low_s[h, :, q, :] = low[:, q * 128 : q * 128 + 128]

    pl.semaphore_wait(bar, 21)
    for d in (2, 1, 3):
        pl.semaphore_signal(known, inc=1, device_id=(row, in_col(d, 0)), device_id_type=MESH)

    l1 = []
    for n, (dz, dy, dk) in enumerate(row_steps):
        to = in_row(dz, dy, dk)
        l1.append(
            copy(low_s.at[to % 2, pl.ds(to // 2 * 2, 2)], low1_r.at[n], l1_ss, l1_rs, (to, col))
        )
        l1[-1].start()
    for n in (7, 8, 9):
        loads[n].wait()
    pair = [
        copy(tok_v.at[:, 1 - core], tokp_v, pair_ss.at[0], pair_rs.at[0], mate),
        copy(wg_v, wgp_v, pair_ss.at[1], pair_rs.at[1], mate),
        copy(wu_v, wup_v, pair_ss.at[2], pair_rs.at[2], mate),
        copy(wd_v, wdp_v, pair_ss.at[3], pair_rs.at[3], mate),
        copy(b_v.at[core], b_v.at[core], pair_ss.at[4], pair_rs.at[4], mate),
    ]
    for n in range(2):
        pair[n].start()
    loads[6].wait()
    b_v[core] = dot(hyper, gb_v[...]).astype(BF16)
    pair[4].start()

    tok = tok_v[:, core].reshape(half, width)
    gate = dot(tok, wg_v[...])
    pair[0].wait_recv()
    pair[1].wait_recv()
    part = half // 32
    units = gate.shape[1]
    gate_s[...] = (gate + dot(tokp_v[...].reshape(half, width), wgp_v[...])).astype(BF16).reshape(4, 8, part, units)

    def peer(dz, dy, sign=1):
        return in_row(dz, dy, 0, sign) // 2

    gs = []
    for n, (dz, dy) in enumerate(chip_steps):
        i = peer(dz, dy)
        gs.append(copy(gate_s.at[:, i], gate_r.at[n], g_ss, g_rs, (i * 2 + core, col)))
    for n, (dz, dy) in enumerate(chip_steps):
        if dz == 0:
            gs[n].start()

    low = low_s[core, pl.ds(chip * 2, 2)]
    all_of(low1_r, l1_ss, l1_rs).wait_recv()
    low = low + jnp.sum(low1_r[...], axis=0)
    low2_s[...] = low
    pl.semaphore_wait(known, 3)
    l2 = []
    for n, (dz, dx) in enumerate(col_steps):
        l2.append(copy(low2_s, low2_r.at[n], l2_ss, l2_rs, (row, in_col(dz, dx))))
        l2[-1].start()
    for n, (dz, dy) in enumerate(chip_steps):
        if dz == 1:
            gs[n].start()
    pair[2].start()
    pair[3].start()

    up = dot(tok, wu_v[...])
    pair[2].wait_recv()
    up_f[...] = up + dot(tokp_v[...].reshape(half, width), wup_v[...])
    pair[4].wait_recv()
    b_all = b_v[...].reshape(2 * groups, units)
    block = half // 2
    mem = [member(core * half + a * block, block) for a in range(2)]
    all_of(low2_r, l2_ss, l2_rs).wait_recv()
    low = low + jnp.sum(low2_r[...], axis=0)
    low = low.astype(BF16).astype(F32)
    us = []
    for q in range(4):
        us.append([])
        for n, (dz, dy) in enumerate(chip_steps):
            i = peer(dz, dy)
            us[q].append(
                copy(up_s.at[q, i], up_r.at[q, n], u_ss, u_rs.at[q], (i * 2 + core, col))
            )
    for q in range(4):
        quarter = slice(q % 2 * 64, q % 2 * 64 + 64)
        spread = jnp.concatenate(
            [mem[q // 2][:, quarter] * low[r, q // 2 : q // 2 + 1, quarter] for r in range(2)], axis=0
        ).astype(BF16)
        up = up_f[q * 64 : q * 64 + 64, :] + dot(spread, b_all, ((0,), (0,)))
        up_s[q] = up.astype(BF16).reshape(8, part, units)
        for c in us[q]:
            c.start()

    all_of(gate_r, g_ss, g_rs).wait_recv()
    hs, ms = [], []

    def hidden(q):
        act = jax.nn.silu(gate_s[q, chip].astype(F32) + jnp.sum(gate_r[:, q].astype(F32), axis=0))
        all_of(up_r.at[q], u_ss, u_rs.at[q]).wait_recv()
        up = up_s[q, chip].astype(F32) + jnp.sum(up_r[q].astype(F32), axis=0)
        hid_v[q, chip] = (act * up).astype(BF16)
        hs.append([])
        for n, (dz, dy) in enumerate(chip_steps):
            hs[q].append(
                copy(
                    hid_v.at[q, chip], hid_v.at[q, chip], h_ss, h_rs.at[q],
                    (peer(dz, dy) * 2 + core, col),
                )
            )
            hs[q][-1].start()

    rows = half // 16

    def partial(q):
        all_of(hid_v.at[q, pl.ds(0, 7)], h_ss, h_rs.at[q]).wait_recv()
        hid = hid_v[q].reshape(8 * part, units)
        for k, w in enumerate((wd_v, wdp_v)):
            mix = dot(hid, w[...]).reshape(4, rows, width)
            mix_f[q, k] = mix
            mix_s[q, k] = mix.astype(BF16)
        ms.append([])
        for n, d in enumerate((2, 1, 3)):
            ms[q].append(
                copy(mix_s.at[q, :, (x + d) % 4], mix_r.at[q, n], m_ss, m_rs.at[q], (row, in_col(0, d)))
            )
            ms[q][-1].start()

    def end(q):
        here = z_hi == q
        all_of(mix_r.at[q], m_ss, m_rs.at[q]).wait_recv()
        end_s[q] = (mix_f[q, :, x] + jnp.sum(mix_r[q].astype(F32), axis=0)).astype(BF16)
        slot = end_r.at[core, z_hi]
        cross = copy(end_s.at[q, 1], slot, e_ss.at[1], e_rs.at[core], (mate[0], q * 4 + x))
        same = copy(end_s.at[q, 0], slot, e_ss.at[0], e_rs.at[core], (row, q * 4 + x))
        pl.when(jnp.logical_not(here))(same.start)
        cross.start()

        @pl.when(here)
        def _():
            end_r[core, z_hi] = end_s[q, 0]

    hidden(0)
    hidden(1)
    hidden(2)
    pair[3].wait_recv()
    partial(0)
    hidden(3)
    partial(1)
    partial(2)
    end(0)
    partial(3)
    end(1)
    end(2)
    end(3)

    for k in range(2):
        pl.when(core == k)(all_of(end_r.at[k, pl.ds(0, 3)], e_ss.at[0], e_rs.at[k]).wait_recv)
        pl.when(core != k)(all_of(end_r.at[k], e_ss.at[0], e_rs.at[k]).wait_recv)
        total = jnp.sum(end_r[k].astype(F32), axis=0)
        out[k * rows : k * rows + rows, :] = total.astype(BF16)

    for c in pair:
        c.wait_send()
    all_of(low1_r, l1_ss, l1_rs).wait_send()
    all_of(low2_r, l2_ss, l2_rs).wait_send()
    all_of(gate_r, g_ss, g_rs).wait_send()
    all_of(up_r, u_ss, u_rs.at[0]).wait_send()
    all_of(hid_v.at[:, pl.ds(0, 7)], h_ss, h_rs.at[0]).wait_send()
    all_of(mix_r, m_ss, m_rs.at[0]).wait_send()
    all_of(end_s.at[pl.ds(0, 3), 0], e_ss.at[0], e_rs.at[0]).wait_send()
    all_of(end_s.at[:, 1], e_ss.at[1], e_rs.at[0]).wait_send()


def shards(tokens, task_emb, gen_in, gen_a, gen_b, w_gate, w_up, w_down, group_count, group_task):
    batch, draft, width = tokens.shape
    hyper, slab, ranks = gen_a.shape
    groups = group_count.shape[0]
    units = w_gate.shape[1]
    n_tok = batch * draft
    half = n_tok // 2
    share = half // 8
    part = half // 32
    rows = half // 16
    vm = pltpu.VMEM
    dma = pltpu.SemaphoreType.DMA
    args = (
        tokens,
        task_emb,
        gen_in,
        gen_a.transpose(1, 2, 0).reshape(slab * ranks, hyper),
        gen_b.reshape(hyper, units),
        w_gate,
        w_up,
        w_down,
        group_count.reshape(1, groups),
        group_task.reshape(1, groups),
    )
    scratch = [vm(a.shape, a.dtype) for a in args]
    scratch += [
        vm((16, 2, rows, width), BF16),
        vm((16, rows, width), BF16),
        vm((width, units), BF16),
        vm((width, units), BF16),
        vm((units, width), BF16),
        vm((2, groups, units), BF16),
        vm((2, ranks, 2, half // 2), F32),
        vm((15, 2, 2, half // 2), F32),
        vm((2, 2, half // 2), F32),
        vm((15, 2, 2, half // 2), F32),
        vm((4, 8, part, units), BF16),
        vm((half, units), F32),
        vm((4, 8, part, units), BF16),
        vm((7, 4, part, units), BF16),
        vm((4, 7, part, units), BF16),
        vm((4, 8, part, units), BF16),
        vm((4, 2, 4, rows, width), F32),
        vm((4, 2, 4, rows, width), BF16),
        vm((4, 3, 2, rows, width), BF16),
        vm((4, 2, rows, width), BF16),
        vm((2, 4, rows, width), BF16),
        pltpu.SemaphoreType.REGULAR,
    ]
    scratch += [dma((10,)), dma((5,)), dma((5,))] + [dma] * 6 + [dma, dma((4,))] * 3 + [dma((2,))] * 2
    any_spec = pl.BlockSpec(memory_space=pl.ANY)
    out = pl.pallas_call(
        kernel,
        out_shape=jax.ShapeDtypeStruct((share, width), BF16),
        in_specs=[any_spec] * len(args),
        out_specs=pl.BlockSpec(memory_space=pltpu.VMEM),
        scratch_shapes=scratch,
        compiler_params=pltpu.CompilerParams(
            collective_id=0, has_side_effects=True, vmem_limit_bytes=32 * 1024 * 1024
        ),
    )(*[pltpu.with_memory_space_constraint(a, pltpu.HBM) for a in args])
    return out.reshape(share // draft, draft, width)


def solution(mesh):
    placed = (
        P(None, None, "row"),
        P(),
        P(),
        P(None, ("row", "col"), None),
        P(None, "row", "col"),
        P("row", "col"),
        P("row", "col"),
        P("col", "row"),
        P(),
        P(),
    )
    return jax.shard_map(
        shards, mesh=mesh, in_specs=placed, out_specs=P("col", None, "row"), check_vma=False
    )
```
